32 devices in a mesh: col: 4 (over y, x), sec: 8 (over z, core).
Axes of the slice: x: 2, y: 2, z: 4, core: 2. Of those that a mesh axis runs over, the one named last changes fastest.
Arguments:
- thermal_state: float32 [128, 64, 256], P('sec', 'col'), may hold values from -6 to 6
- flow_vector: float32 [2, 128, 64, 256], P(None, 'sec', 'col'), may hold values from -5 to 5
- vertical_spreading: float32 [128, 64, 256], P('sec', 'col'), may hold values from 0.05 to 0.5
- solute_fields: float32 [32, 128, 64, 256], P('sec', None, 'col'), may hold values from 0.1 to 2
- linear_exchange_speeds: float32 [32, 32], replicated, may hold values from -1 to 1
- newton_preconditioner: float32 [32, 32], replicated, may hold values from -0.6 to 1.2
- absorption_speed: float32 [32], replicated, may hold values from 0.2 to 2
- water_indicator: int32 [64, 256], P('col'), may hold values from 0 to 1, as said below
Outputs:
- thermal_revised: float32 [128, 64, 256], P('sec', 'col')
- velocity_next: float32 [2, 128, 64, 256], P(None, 'sec', 'col')
- diffusivity_next: float32 [128, 64, 256], P('sec', 'col')
- solute_revised: float32 [32, 128, 64, 256], P('sec', None, 'col')
The draws below stay inside these ranges and needn't reach their ends.
Inputs may be any that keep to these rules, and one draw needn't show every extreme that they name: `water_indicator`: in each block of 16 consecutive longitudes, between 1536 and 3072 columns are wet, and some block holds exactly 3072 wet columns.
All inputs are finite; a program needn't handle non-finite values.
Results may differ from the reference program's by a relative error of at most 0.0001.
Values sent between devices are 32-bit elements; how exact they have to be, the bound alone decides.
No kernel may reach another device: no remote copies, remote signals or barrier semaphores. Data moves between devices by JAX's collectives and lax.ppermute only.
A program may use at most 128 MiB of HBM per device.

```python
import math
import jax
import jax.numpy as jnp
from jax import lax

XD = 16
PARALLEL_TOTAL = 256
LAYER_TOTAL = 128
NTR = 32
NEWTON = 2
MERIDIAN_TOTAL = 64


def draw_newton_preconditioner(key, part):
    spread = 0.25 * jax.random.normal(jax.random.fold_in(key, 11), (NTR, NTR), jnp.float32)
    spread = jnp.clip(spread / jnp.sqrt(NTR * 1.0), -0.55, 0.55)
    return (0.6 * jnp.eye(NTR, dtype=jnp.float32) + spread).astype(jnp.float32)


def draw_water_indicator(key, part):
    blocks = MERIDIAN_TOTAL // XD
    columns = XD * PARALLEL_TOTAL
    most = 3 * columns // 4
    counts = jax.random.randint(jax.random.fold_in(key, 21), (blocks,), most // 2, most + 1)
    fullest = jax.random.randint(jax.random.fold_in(key, 22), (), 0, blocks)
    counts = jnp.where(jnp.arange(blocks) == fullest, most, counts)
    ranks = jax.vmap(lambda sub: jax.random.permutation(sub, columns))(jax.random.split(jax.random.fold_in(key, 23), blocks))
    return (ranks < counts[:, None]).astype(jnp.int32).reshape(MERIDIAN_TOTAL, PARALLEL_TOTAL)


def levels(stream_key, dims, pieces, low, top_value):
    def one(axis_at, blocks):
        draws = jax.random.uniform(jax.random.fold_in(jax.random.fold_in(stream_key, 6), axis_at), (blocks,), jnp.float32, low / len(pieces), top_value / len(pieces))
        return jnp.repeat(jnp.exp(draws), dims[axis_at] // blocks).reshape((-1,) + (1,) * (len(dims) - axis_at - 1))

    level = one(*pieces[0])
    for cut in pieces[1:]:
        level = level * one(*cut)
    return level


def noise(stream_key, shape, scale, reach, shards=(), kind=jnp.bfloat16):
    entries = jax.random.normal(stream_key, shape, jnp.float32) * scale
    if len(shards) > 0:
        entries = levels(stream_key, shape, shards, -0.22, 0.18) * entries
    return jnp.clip(entries, min=-reach, max=reach).astype(kind)


def setup_inputs(seed: int = 0) -> dict:
    splits = jax.random.split(jax.random.key(seed), 9)
    thermal_state = noise(splits[0], (LAYER_TOTAL, MERIDIAN_TOTAL, PARALLEL_TOTAL), 1.0, 6.0, ((0, 8), (1, 4)), jnp.float32)
    flow_vector = noise(splits[1], (2, LAYER_TOTAL, MERIDIAN_TOTAL, PARALLEL_TOTAL), 1.0, 5.0, ((1, 8), (2, 4)), jnp.float32)
    vertical_spreading = jnp.clip(jnp.exp(math.log(0.5) - 2.3025851 * jax.random.uniform(splits[2], (LAYER_TOTAL, MERIDIAN_TOTAL, PARALLEL_TOTAL), jnp.float32) ** levels(splits[2], (LAYER_TOTAL, MERIDIAN_TOTAL, PARALLEL_TOTAL), ((0, 8), (1, 4)), -0.2, 0.2)), 0.05, 0.5)
    solute_fields = jnp.clip(jnp.exp(math.log(2.0) - 2.9957323 * jax.random.uniform(splits[3], (NTR, LAYER_TOTAL, MERIDIAN_TOTAL, PARALLEL_TOTAL), jnp.float32) ** levels(splits[3], (NTR, LAYER_TOTAL, MERIDIAN_TOTAL, PARALLEL_TOTAL), ((0, 8), (2, 4)), -0.2, 0.2)), 0.1, 2.0)
    linear_exchange_speeds = noise(splits[4], (NTR, NTR), NTR ** -0.5, 1.0, (), jnp.float32)
    newton_preconditioner = draw_newton_preconditioner(jax.random.fold_in(splits[8], 71), 0)
    absorption_speed = jnp.clip(jnp.exp(jax.random.uniform(splits[6], (NTR,), jnp.float32, math.log(0.2), math.log(2.0))), 0.2, 2.0)
    water_indicator = draw_water_indicator(jax.random.fold_in(splits[8], 71), 0)
    return dict(thermal_state=thermal_state, flow_vector=flow_vector, vertical_spreading=vertical_spreading, solute_fields=solute_fields, linear_exchange_speeds=linear_exchange_speeds, newton_preconditioner=newton_preconditioner, absorption_speed=absorption_speed, water_indicator=water_indicator)


CORIOLIS = 0.8
MIXING = 0.1
ADVECTION = 0.2
VERTICAL_MIX = 0.3
WATER_ABSORB = 0.02
PIGMENT_ABSORB = 0.06
CHLOROPHYLL_WARM = 10.0


def latitude_terms(count):
    index = jnp.arange(count).astype(jnp.float32)
    latitude = jnp.pi * (index + 0.5) / count - jnp.pi / 2
    return jnp.sin(latitude), jnp.cos(latitude)


def chemical_change(center, eastern, western, east_flow, north_flow):
    northern = jnp.concatenate([center[..., 1:], center[..., -1:]], axis=-1)
    southern = jnp.concatenate([center[..., :1], center[..., :-1]], axis=-1)
    laplace = eastern + western + northern + southern - 4.0 * center
    return MIXING * laplace - 0.5 * ADVECTION * (east_flow * (eastern - western) + north_flow * (northern - southern))


def column_mixing(field, kappa):
    weights = VERTICAL_MIX * kappa[:-1]
    fluxes = weights[None] * (field[:, 1:] - field[:, :-1])
    zeros = jnp.zeros_like(fluxes[:, :1])
    return jnp.concatenate([fluxes, zeros], axis=1) - jnp.concatenate([zeros, fluxes], axis=1)


def react(start, linear_exchange_speeds, newton_preconditioner, absorption_speed):
    rates = absorption_speed.reshape((-1,) + (1,) * (start.ndim - 1))
    current = start
    for step in range(NEWTON):
        linear = jnp.einsum("ij,j...->i...", linear_exchange_speeds, current, precision=lax.Precision.HIGHEST)
        square = current * current
        rate = linear - rates * square / (1.0 + square)
        misfit = current - start - rate
        current = current - jnp.einsum("ij,j...->i...", newton_preconditioner, misfit, precision=lax.Precision.HIGHEST)
    return current


def heating(pigment_tracer, shortwave):
    square = pigment_tracer * pigment_tracer
    absorb = WATER_ABSORB + PIGMENT_ABSORB * square / (1.0 + square)
    depth = jnp.cumsum(absorb, axis=0)
    return shortwave * (jnp.exp(-(depth - absorb)) - jnp.exp(-depth))


def reference(thermal_state, flow_vector, vertical_spreading, solute_fields, linear_exchange_speeds, newton_preconditioner, absorption_speed, water_indicator):
    sines, cosines = latitude_terms(PARALLEL_TOTAL)
    rotation = CORIOLIS * sines
    divisor = 1.0 + rotation * rotation
    zonal_flow_speed = (flow_vector[0] + rotation * flow_vector[1]) / divisor
    meridional_flow_speed = (flow_vector[1] - rotation * flow_vector[0]) / divisor
    zero_level = jnp.zeros_like(zonal_flow_speed[:1])
    east_below = jnp.concatenate([zonal_flow_speed[1:], zero_level], axis=0)
    north_below = jnp.concatenate([meridional_flow_speed[1:], zero_level], axis=0)
    shear = (zonal_flow_speed - east_below) ** 2 + (meridional_flow_speed - north_below) ** 2
    spreading_revised = 0.5 * vertical_spreading + 0.5 * shear / (1.0 + shear)
    thermal_carried = thermal_state + chemical_change(thermal_state, jnp.roll(thermal_state, -1, axis=1), jnp.roll(thermal_state, 1, axis=1), zonal_flow_speed, meridional_flow_speed)
    water_sites = water_indicator.astype(jnp.float32)
    moved = solute_fields + water_sites * (chemical_change(solute_fields, jnp.roll(solute_fields, -1, axis=2), jnp.roll(solute_fields, 1, axis=2), zonal_flow_speed, meridional_flow_speed) + column_mixing(solute_fields, spreading_revised))
    reacted = react(moved, linear_exchange_speeds, newton_preconditioner, absorption_speed)
    solute_revised = jnp.where(water_indicator > 0, reacted, moved)
    warming_quantity = heating(solute_revised[0], cosines)
    thermal_revised = thermal_carried + CHLOROPHYLL_WARM * water_sites * warming_quantity
    return thermal_revised, jnp.stack([zonal_flow_speed, meridional_flow_speed]), spreading_revised, solute_revised
```

```python
import functools

import jax
import jax.numpy as jnp
from jax import lax
from jax.experimental import pallas as pl
from jax.experimental.pallas import tpu as pltpu
from jax.sharding import PartitionSpec as P

NEWTON = 2
CORIOLIS = 0.8
MIXING = 0.1
ADVECTION = 0.2
VERTICAL_MIX = 0.3
WATER_ABSORB = 0.02
PIGMENT_ABSORB = 0.06
CHLOROPHYLL_WARM = 10.0
LANES = 128
ROWS = 8


def shifted(block, axis, distance):
    devices = range(lax.axis_size(axis))
    route = [(i - distance, i) for i in devices if i - distance in devices]
    return lax.ppermute(block, axis, route)


def around(block, axis, distance):
    count = lax.axis_size(axis)
    return lax.ppermute(block, axis, [(i, (i + distance) % count) for i in range(count)])


def chemical_change(center, eastern, western, east_flow, north_flow):
    northern = jnp.concatenate([center[..., 1:], center[..., -1:]], axis=-1)
    southern = jnp.concatenate([center[..., :1], center[..., :-1]], axis=-1)
    laplace = eastern + western + northern + southern - 4.0 * center
    return MIXING * laplace - 0.5 * ADVECTION * (
        east_flow * (eastern - western) + north_flow * (northern - southern)
    )


def react_kernel(n, nl, q, *refs):
    me_ref, tile_ref, shift_ref = refs[:3]
    cur = refs[3 : 3 + n]
    below = refs[3 + n : 3 + 2 * n]
    above = refs[3 + 2 * n : 3 + 3 * n]
    rest = refs[3 + 3 * n :]
    east_halo, west_halo, east, north, kmix, water, speeds, precon, rates, pick = rest[:10]
    outs = rest[10 : 10 + n]
    pigment = rest[10 + n]
    moved, done, packed = rest[11 + n :]
    held, _, across, lat = cur[0].shape
    tracers = n * held
    halves = across // ROWS
    rows = tracers * ROWS

    row_at = lax.broadcasted_iota(jnp.int32, (across, lat), 0)
    lane_at = lax.broadcasted_iota(jnp.int32, (across, lat), 1)
    wet = water[...]
    for l in range(nl):
        u = (0.5 * ADVECTION) * wet * east[l]
        v = (0.5 * ADVECTION) * wet * north[l]
        mix = MIXING * wet
        up = wet * kmix[q * nl + l + 1]
        down = wet * kmix[q * nl + l]
        to_east = mix - u
        to_west = mix + u
        last = lane_at == lat - 1
        first = lane_at == 0
        middle = 1.0 - 4.0 * mix - up - down
        to_north = mix - v
        to_south = mix + v
        middle = middle + jnp.where(last, to_north, 0.0) + jnp.where(first, to_south, 0.0)
        to_north = jnp.where(last, 0.0, to_north)
        to_south = jnp.where(first, 0.0, to_south)
        for d in range(n):
            for i in range(held):
                t = d * held + i
                c = cur[d][i, l]
                lower = cur[d][i, l - 1] if l > 0 else below[d][i, 0]
                upper = cur[d][i, l + 1] if l < nl - 1 else above[d][i, 0]
                at = t * nl + l
                e = jnp.where(
                    row_at == across - 1, east_halo[at : at + 1, :], pltpu.roll(c, across - 1, 0)
                )
                w = jnp.where(row_at == 0, west_halo[at : at + 1, :], pltpu.roll(c, 1, 0))
                value = middle * c + to_east * e + to_west * w
                value = value + to_north * pltpu.roll(c, lat - 1, 1) + to_south * pltpu.roll(c, 1, 1)
                value = value + up * upper + down * lower
                for h in range(halves):
                    moved[l * halves + h, t * ROWS : (t + 1) * ROWS, :] = value[
                        h * ROWS : (h + 1) * ROWS
                    ]

    def product(weights, x):
        high = x.astype(jnp.bfloat16)
        low = (x - high.astype(jnp.float32)).astype(jnp.bfloat16)
        return jnp.dot(
            weights[...],
            jnp.concatenate([high, low, high], axis=0),
            preferred_element_type=jnp.float32,
        )

    def uptake(x):
        square = x * x
        return rates[...] * (square / (1.0 + square))

    def react(j, carry):
        start = moved[j]
        current = start
        for step in range(NEWTON):
            misfit = uptake(current) - product(speeds, current)
            if step > 0:
                misfit = misfit + (current - start)
            current = current - product(precon, misfit)
        l = j // halves
        h = j % halves
        for t in range(tracers):
            at = pl.multiple_of((t * nl + l) * across + h * ROWS, ROWS)
            for s in range(lat // LANES):
                done[s, pl.ds(at, ROWS), :] = current[
                    t * ROWS : (t + 1) * ROWS, s * LANES : (s + 1) * LANES
                ]
        return carry

    lax.fori_loop(0, nl * halves, react, 0)

    me = me_ref[0]
    for l in range(nl):
        at = pl.multiple_of((me * (held * nl) + l) * across, ROWS)
        for s in range(lat // LANES):
            pigment[l, :, s * LANES : (s + 1) * LANES] = done[s, pl.ds(at, across), :]

    lane = lax.broadcasted_iota(jnp.int32, (ROWS, LANES), 1)
    parts = lat // LANES

    def pack(x, carry):
        for s in range(parts):
            segment = x * parts + s
            tile = pl.multiple_of(tile_ref[segment] * LANES, LANES)
            tail = pl.multiple_of(tile_ref[segment] * LANES + LANES, LANES)
            keep = lane < shift_ref[segment]
            index = jnp.broadcast_to(pick[pl.ds(segment, 1), :], (ROWS, LANES))
            for g in range(tracers * nl // ROWS):
                value = done[s, pl.ds(g * ROWS * across + x, ROWS, stride=across), :]
                value = jnp.take_along_axis(value, index, axis=1, mode="promise_in_bounds")
                here = (slice(g * ROWS, (g + 1) * ROWS), pl.ds(tile, LANES))
                packed[here] = jnp.where(keep, packed[here], value)
                packed[g * ROWS : (g + 1) * ROWS, pl.ds(tail, LANES)] = value
        return carry

    lax.fori_loop(0, across, pack, 0)
    for d in range(n):
        outs[d][...] = packed[d * held * nl : (d + 1) * held * nl, : outs[d].shape[1]]


def react_chunk(q, nl, me, tiles, shifts, blocks, below, above, halos, fields, cap):
    n = len(blocks)
    held, _, across, lat = blocks[0].shape
    east, north, kmix, water, speeds, precon, rates, pick = fields
    rows = n * held * ROWS
    whole = pl.BlockSpec(memory_space=pltpu.VMEM)

    def level(spec_at):
        return pl.BlockSpec((held, 1, across, lat), lambda i, *_: (0, spec_at, 0, 0))

    def all_of(x):
        return pl.BlockSpec(x.shape, lambda i, *_: (0,) * x.ndim)

    ins = list(blocks)
    specs = [all_of(b) for b in blocks]
    for source, at in (below, above):
        for d in range(n):
            if isinstance(source, list):
                ins.append(source[d])
                specs.append(level(at))
            else:
                ins.append(source)
                specs.append(
                    pl.BlockSpec((held, 1, across, lat), lambda i, *_, d=d: (d, 0, 0, 0))
                )
    for x in halos:
        ins.append(x)
        specs.append(all_of(x))
    for x in (east, north):
        ins.append(x)
        specs.append(pl.BlockSpec((nl, across, lat), lambda i, *_: (q, 0, 0)))
    for x in (kmix, water, speeds, precon, rates, pick):
        ins.append(x)
        specs.append(all_of(x))
    out_block = jax.ShapeDtypeStruct((held * nl, cap), jnp.float32)
    shapes = [out_block] * n + [jax.ShapeDtypeStruct((nl, across, lat), jnp.float32)]
    lanes = (cap // LANES + 2) * LANES
    flops = 2 * 12 * rows * rows * lat * nl * (across // ROWS)
    return pl.pallas_call(
        functools.partial(react_kernel, n, nl, q),
        grid_spec=pltpu.PrefetchScalarGridSpec(
            num_scalar_prefetch=3,
            grid=(1,),
            in_specs=specs,
            out_specs=[
                pl.BlockSpec(s.shape, lambda i, *_, k=len(s.shape): (0,) * k) for s in shapes
            ],
            scratch_shapes=[
                pltpu.VMEM((nl * (across // ROWS), rows, lat), jnp.float32),
                pltpu.VMEM((lat // LANES, n * held * nl * across, LANES), jnp.float32),
                pltpu.VMEM((n * held * nl, lanes), jnp.float32),
            ],
        ),
        out_shape=shapes,
        cost_estimate=pl.CostEstimate(
            flops=flops, bytes_accessed=4 * 3 * rows * nl * across * lat // ROWS, transcendentals=0
        ),
        name="react",
    )(me, tiles, shifts, *ins)


def unpack_kernel(n, has_base, *refs):
    me_ref, tile_ref = refs[:2]
    received = refs[2 : 2 + n]
    solute, water, pick, second = refs[2 + n : 6 + n]
    out, slots, spread = refs[6 + n + has_base :]
    held, nl, across, lat = solute.shape
    cap = received[0].shape[1]
    d = pl.program_id(0)
    for k in range(n):

        @pl.when(d == k)
        def _():
            slots[:, :cap] = received[k][...]

    parts = lat // LANES
    for x in range(across):
        for s in range(parts):
            segment = x * parts + s
            tile = pl.multiple_of(tile_ref[segment] * LANES, LANES)
            tail = pl.multiple_of(tile_ref[segment] * LANES + LANES, LANES)
            index = jnp.broadcast_to(pick[segment : segment + 1, :], (ROWS, LANES))
            later = jnp.broadcast_to(second[segment : segment + 1, :], (ROWS, LANES)) > 0
            for g in range(held * nl // ROWS):
                group = slice(g * ROWS, (g + 1) * ROWS)
                a = jnp.take_along_axis(
                    slots[group, pl.ds(tile, LANES)], index, axis=1, mode="promise_in_bounds"
                )
                b = jnp.take_along_axis(
                    slots[group, pl.ds(tail, LANES)], index, axis=1, mode="promise_in_bounds"
                )
                spread[s, pl.ds(g * ROWS * across + x, ROWS, stride=across), :] = jnp.where(
                    later, b, a
                )
    wet = water[...] > 0.5
    for i in range(held):
        for l in range(nl):
            at = (i * nl + l) * across
            for s in range(parts):
                lanes = slice(s * LANES, (s + 1) * LANES)
                out[i, l, :, lanes] = jnp.where(
                    wet[:, lanes], spread[s, at : at + across, :], solute[i, l, :, lanes]
                )


def unpack_chunk(q, parts, me, tiles, received, solute, water, pick, second, base):
    n = len(received)
    held, depth, across, lat = solute.shape
    nl = depth // n // parts
    cap = received[0].shape[1]

    def all_of(x):
        return pl.BlockSpec(x.shape, lambda d, *_: (0,) * x.ndim)

    place = pl.BlockSpec(
        (held, nl, across, lat), lambda d, me, *_: (0, lax.rem(me[0] + d, n) * parts + q, 0, 0)
    )
    specs = [all_of(x) for x in received] + [place, all_of(water), all_of(pick), all_of(second)]
    ins = [*received, solute, water, pick, second]
    aliases = {}
    if base is not None:
        aliases = {2 + len(ins): 0}
        ins.append(base)
        specs.append(pl.BlockSpec(memory_space=pl.ANY))
    return pl.pallas_call(
        functools.partial(unpack_kernel, n, base is not None),
        grid_spec=pltpu.PrefetchScalarGridSpec(
            num_scalar_prefetch=2,
            grid=(n,),
            in_specs=specs,
            out_specs=place,
            scratch_shapes=[
                pltpu.VMEM((held * nl, (cap // LANES + 2) * LANES), jnp.float32),
                pltpu.VMEM((lat // LANES, held * nl * across, LANES), jnp.float32),
            ],
        ),
        out_shape=jax.ShapeDtypeStruct(solute.shape, jnp.float32),
        input_output_aliases=aliases,
        cost_estimate=pl.CostEstimate(
            flops=100 * solute.size, bytes_accessed=12 * solute.size // parts, transcendentals=0
        ),
        name="unpack",
    )(me, tiles, *ins)


def relative(x, me, n, axis):
    x = jnp.flip(x, axis)
    return lax.dynamic_slice_in_dim(jnp.concatenate([x, x], axis), n - 1 - me, n, axis)


def halves_of(x):
    high = lax.reduce_precision(x, 8, 7)
    low = x - high
    return jnp.concatenate([high, high, low], axis=1).astype(jnp.bfloat16)


def on_device(
    thermal_state,
    flow_vector,
    vertical_spreading,
    solute_fields,
    linear_exchange_speeds,
    newton_preconditioner,
    absorption_speed,
    water_indicator,
):
    n = lax.axis_size("sec")
    me = lax.axis_index("sec")
    held, depth, across, lat = solute_fields.shape
    tracers = n * held
    levels = depth // n
    nl = max(levels // 4, ROWS // held)
    parts = levels // nl
    order = [0, parts - 1, *range(1, parts - 1)] if parts > 1 else [0]
    me_at = jnp.reshape(me, (1,)).astype(jnp.int32)

    blocks = {}
    for q in order:
        blocks[q] = []
        for d in range(n):
            to = lax.rem(me + d, n)
            block = lax.dynamic_slice_in_dim(solute_fields, to * levels + q * nl, nl, 1)
            blocks[q].append(around(block, "sec", d) if d else block)

    latitude = jnp.pi * (jnp.arange(lat).astype(jnp.float32) + 0.5) / lat - jnp.pi / 2
    rotation = CORIOLIS * jnp.sin(latitude)
    shortwave = jnp.cos(latitude)
    divisor = 1.0 + rotation * rotation
    east = (flow_vector[0] + rotation * flow_vector[1]) / divisor
    north = (flow_vector[1] - rotation * flow_vector[0]) / divisor
    top_level = shifted(jnp.stack([east[0], north[0]]), "sec", -1)
    east_below = jnp.concatenate([east[1:], top_level[:1]], axis=0)
    north_below = jnp.concatenate([north[1:], top_level[1:]], axis=0)
    shear = (east - east_below) ** 2 + (north - north_below) ** 2
    spreading = 0.5 * vertical_spreading + 0.5 * shear / (1.0 + shear)
    level_at = me * levels + jnp.arange(levels)
    kmix = jnp.where((level_at < depth - 1)[:, None, None], VERTICAL_MIX * spreading, 0.0)
    kmix = jnp.concatenate([shifted(kmix[-1:], "sec", 1), kmix], axis=0)
    thermal_west = around(thermal_state[:, -1:], "col", 1)
    thermal_east = around(thermal_state[:, :1], "col", -1)
    thermal_carried = thermal_state + chemical_change(
        thermal_state,
        jnp.concatenate([thermal_state[:, 1:], thermal_east], axis=1),
        jnp.concatenate([thermal_west, thermal_state[:, :-1]], axis=1),
        east,
        north,
    )

    water = water_indicator.astype(jnp.float32)
    cap = -(-3 * across * lat // 4 // LANES) * LANES
    wet = (water_indicator > 0).astype(jnp.int32).reshape(-1, LANES)
    within = jnp.cumsum(wet, axis=1) - wet
    count = jnp.sum(wet, axis=1)
    offset = jnp.cumsum(count) - count
    tiles = offset // LANES
    shifts = offset % LANES
    slot = within + shifts[:, None]
    lane = jnp.arange(LANES, dtype=jnp.int32)
    hit = (slot % LANES)[:, None, :] == lane[None, :, None]
    gather = jnp.sum(
        jnp.where(hit & (wet > 0)[:, None, :], lane[None, None, :], 0), axis=2, dtype=jnp.int32
    )
    spread_at = slot % LANES
    spread_later = slot // LANES

    speeds = linear_exchange_speeds.reshape(n, held, n, held)
    precon = newton_preconditioner.reshape(n, held, n, held)
    speeds = relative(relative(speeds, me, n, 0), me, n, 2).reshape(tracers, tracers)
    precon = relative(relative(precon, me, n, 0), me, n, 2).reshape(tracers, tracers)
    rates = relative(absorption_speed.reshape(n, held), me, n, 0).reshape(tracers)
    eye = jnp.eye(ROWS, dtype=jnp.float32)
    speeds = halves_of(jnp.kron(speeds, eye))
    precon = halves_of(jnp.kron(precon, eye))
    rates = jnp.broadcast_to(jnp.repeat(rates, ROWS)[:, None], (tracers * ROWS, lat))

    first = jnp.concatenate([blocks[0][(d + 1) % n][:, :1] for d in range(n)], axis=0)
    last = jnp.concatenate([blocks[parts - 1][(d - 1) % n][:, -1:] for d in range(n)], axis=0)
    above_all = shifted(first, "sec", -1)
    below_all = shifted(last, "sec", 1)

    fields = (east, north, kmix, water, speeds, precon, rates, gather)
    pigments = {}
    solute_revised = None
    returned = {}
    for q in order:
        head = jnp.concatenate([b[:, :, 0].reshape(held * nl, lat) for b in blocks[q]], axis=0)
        tail = jnp.concatenate([b[:, :, -1].reshape(held * nl, lat) for b in blocks[q]], axis=0)
        halos = (around(head, "col", -1), around(tail, "col", 1))
        below = (blocks[q - 1], nl - 1) if q > 0 else (below_all, 0)
        above = (blocks[q + 1], 0) if q < parts - 1 else (above_all, 0)
        *packed, pigments[q] = react_chunk(
            q, nl, me_at, tiles, shifts, blocks[q], below, above, halos, fields, cap
        )
        returned[q] = [around(x, "sec", -d) if d else x for d, x in enumerate(packed)]

    for q in order:
        solute_revised = unpack_chunk(
            q, parts, me_at, tiles, returned[q], solute_fields, water, spread_at, spread_later,
            solute_revised,
        )

    pigment = jnp.concatenate([pigments[q] for q in range(parts)], axis=0)
    square = pigment * pigment
    absorb = WATER_ABSORB + PIGMENT_ABSORB * square / (1.0 + square)
    depth_here = jnp.cumsum(absorb, axis=0)
    total = depth_here[-1]
    over = sum(shifted(total, "sec", d) for d in range(1, n))
    depth_to = over[None] + depth_here
    warming = shortwave * (jnp.exp(-(depth_to - absorb)) - jnp.exp(-depth_to))
    thermal_revised = thermal_carried + CHLOROPHYLL_WARM * water * warming
    return thermal_revised, jnp.stack([east, north]), spreading, solute_revised


def solution(mesh):
    placed = (
        P("sec", "col", None),
        P(None, "sec", "col", None),
        P("sec", "col", None),
        P("sec", None, "col", None),
        P(),
        P(),
        P(),
        P("col", None),
    )
    return jax.shard_map(
        on_device,
        mesh=mesh,
        in_specs=placed,
        out_specs=(
            P("sec", "col", None),
            P(None, "sec", "col", None),
            P("sec", "col", None),
            P("sec", None, "col", None),
        ),
        check_vma=False,
    )
```

```python
import functools

import jax
import jax.numpy as jnp
from jax import lax
from jax.experimental import pallas as pl
from jax.experimental.pallas import tpu as pltpu
from jax.sharding import PartitionSpec as P


NEWTON = 2
CORIOLIS = 0.8
MIXING = 0.1
ADVECTION = 0.2
VERTICAL_MIX = 0.3
WATER_ABSORB = 0.02
PIGMENT_ABSORB = 0.06
CHLOROPHYLL_WARM = 10.0
LANES = 128
ROWS = 8


def shifted(block, axis, distance):
    devices = range(lax.axis_size(axis))
    route = [(i - distance, i) for i in devices if i - distance in devices]
    return lax.ppermute(block, axis, route)


def around(block, axis, distance):
    count = lax.axis_size(axis)
    return lax.ppermute(block, axis, [(i, (i + distance) % count) for i in range(count)])


def chemical_change(center, eastern, western, east_flow, north_flow):
    northern = jnp.concatenate([center[..., 1:], center[..., -1:]], axis=-1)
    southern = jnp.concatenate([center[..., :1], center[..., :-1]], axis=-1)
    laplace = eastern + western + northern + southern - 4.0 * center
    return MIXING * laplace - 0.5 * ADVECTION * (
        east_flow * (eastern - western) + north_flow * (northern - southern)
    )


def edges_kernel(n, level, turn, *refs):
    cur = refs[:n]
    head, tail = refs[n : n + 2]
    held, nl, across, _ = cur[0].shape
    for d in range(n):
        for i in range(held):
            for l in range(nl):
                at = (d * held + i) * nl + l
                head[at : at + 1, :] = cur[d][i, l, 0:1, :]
                tail[at : at + 1, :] = cur[d][i, l, across - 1 : across, :]
    if level is not None:
        for d in range(n):
            refs[n + 2][d * held : (d + 1) * held] = cur[(d + turn) % n][:, level : level + 1]


def chunk_edges(blocks, level, turn):
    n = len(blocks)
    held, nl, across, lat = blocks[0].shape
    shapes = [jax.ShapeDtypeStruct((n * held * nl, lat), jnp.float32)] * 2
    if level is not None:
        shapes.append(jax.ShapeDtypeStruct((n * held, 1, across, lat), jnp.float32))
    return pl.pallas_call(
        functools.partial(edges_kernel, n, level, turn),
        in_specs=[pl.BlockSpec(memory_space=pltpu.VMEM)] * n,
        out_specs=[pl.BlockSpec(memory_space=pltpu.VMEM)] * len(shapes),
        out_shape=shapes,
        cost_estimate=pl.CostEstimate(
            flops=10**8, bytes_accessed=4 * n * blocks[0].size, transcendentals=0
        ),
        name="edges",
    )(*blocks)


def react_kernel(n, nl, q, *refs):
    me_ref, tile_ref, shift_ref = refs[:3]
    cur = refs[3 : 3 + n]
    below = refs[3 + n : 3 + 2 * n]
    above = refs[3 + 2 * n : 3 + 3 * n]
    rest = refs[3 + 3 * n :]
    east_halo, west_halo, east, north, kmix, water, speeds, precon, rates, pick = rest[:10]
    outs = rest[10 : 10 + n]
    pigment = rest[10 + n]
    moved, done, packed = rest[11 + n :]
    held, _, across, lat = cur[0].shape
    tracers = n * held
    halves = across // ROWS

    row_at = lax.broadcasted_iota(jnp.int32, (across, lat), 0)
    lane_at = lax.broadcasted_iota(jnp.int32, (across, lat), 1)
    wet = water[...]
    for l in range(nl):
        u = (0.5 * ADVECTION) * wet * east[l]
        v = (0.5 * ADVECTION) * wet * north[l]
        mix = MIXING * wet
        up = wet * kmix[q * nl + l + 1]
        down = wet * kmix[q * nl + l]
        to_east = mix - u
        to_west = mix + u
        last = lane_at == lat - 1
        first = lane_at == 0
        middle = 1.0 - 4.0 * mix - up - down
        to_north = mix - v
        to_south = mix + v
        middle = middle + jnp.where(last, to_north, 0.0) + jnp.where(first, to_south, 0.0)
        to_north = jnp.where(last, 0.0, to_north)
        to_south = jnp.where(first, 0.0, to_south)
        for d in range(n):
            for i in range(held):
                t = d * held + i
                c = cur[d][i, l]
                lower = cur[d][i, l - 1] if l > 0 else below[d][i, 0]
                upper = cur[d][i, l + 1] if l < nl - 1 else above[d][i, 0]
                at = t * nl + l
                e = jnp.where(
                    row_at == across - 1, east_halo[at : at + 1, :], pltpu.roll(c, across - 1, 0)
                )
                w = jnp.where(row_at == 0, west_halo[at : at + 1, :], pltpu.roll(c, 1, 0))
                value = middle * c + to_east * e + to_west * w
                value = value + to_north * pltpu.roll(c, lat - 1, 1) + to_south * pltpu.roll(c, 1, 1)
                value = value + up * upper + down * lower
                for h in range(halves):
                    moved[l * halves + h, t * ROWS : (t + 1) * ROWS, :] = value[
                        h * ROWS : (h + 1) * ROWS
                    ]

    def product(weights, x):
        high = x.astype(jnp.bfloat16)
        low = (x - high.astype(jnp.float32)).astype(jnp.bfloat16)
        return jnp.dot(
            weights[...],
            jnp.concatenate([high, low, high], axis=0),
            preferred_element_type=jnp.float32,
        )

    def uptake(x):
        square = x * x
        return rates[...] * (square / (1.0 + square))

    def react(j, carry):
        start = moved[j]
        current = start
        for step in range(NEWTON):
            misfit = uptake(current) - product(speeds, current)
            if step > 0:
                misfit = misfit + (current - start)
            current = current - product(precon, misfit)
        l = j // halves
        h = j % halves
        for t in range(tracers):
            at = pl.multiple_of((t * nl + l) * across + h * ROWS, ROWS)
            for s in range(lat // LANES):
                done[s, pl.ds(at, ROWS), :] = current[
                    t * ROWS : (t + 1) * ROWS, s * LANES : (s + 1) * LANES
                ]
        return carry

    lax.fori_loop(0, nl * halves, react, 0)

    me = me_ref[0]
    for l in range(nl):
        at = pl.multiple_of((me * (held * nl) + l) * across, ROWS)
        for s in range(lat // LANES):
            pigment[l, :, s * LANES : (s + 1) * LANES] = done[s, pl.ds(at, across), :]

    lane = lax.broadcasted_iota(jnp.int32, (ROWS, LANES), 1)
    parts = lat // LANES

    def pack(x, carry):
        for s in range(parts):
            segment = x * parts + s
            tile = pl.multiple_of(tile_ref[segment] * LANES, LANES)
            tail = pl.multiple_of(tile_ref[segment] * LANES + LANES, LANES)
            keep = lane < shift_ref[segment]
            index = jnp.broadcast_to(pick[pl.ds(segment, 1), :], (ROWS, LANES))
            for g in range(tracers * nl // ROWS):
                value = done[s, pl.ds(g * ROWS * across + x, ROWS, stride=across), :]
                value = jnp.take_along_axis(value, index, axis=1, mode="promise_in_bounds")
                here = (slice(g * ROWS, (g + 1) * ROWS), pl.ds(tile, LANES))
                packed[here] = jnp.where(keep, packed[here], value)
                packed[g * ROWS : (g + 1) * ROWS, pl.ds(tail, LANES)] = value
        return carry

    lax.fori_loop(0, across, pack, 0)
    for d in range(n):
        outs[d][...] = packed[d * held * nl : (d + 1) * held * nl, : outs[d].shape[1]]


def react_chunk(q, nl, me, tiles, shifts, blocks, below, above, halos, fields, cap):
    n = len(blocks)
    held, _, across, lat = blocks[0].shape
    east, north, kmix, water, speeds, precon, rates, pick = fields
    rows = n * held * ROWS
    whole = pl.BlockSpec(memory_space=pltpu.VMEM)

    def level(spec_at):
        return pl.BlockSpec((held, 1, across, lat), lambda i, *_: (0, spec_at, 0, 0))

    def all_of(x):
        return pl.BlockSpec(x.shape, lambda i, *_: (0,) * x.ndim)

    ins = list(blocks)
    specs = [all_of(b) for b in blocks]
    for source, at in (below, above):
        for d in range(n):
            if isinstance(source, list):
                ins.append(source[d])
                specs.append(level(at))
            else:
                ins.append(source)
                specs.append(
                    pl.BlockSpec((held, 1, across, lat), lambda i, *_, d=d: (d, 0, 0, 0))
                )
    for x in halos:
        ins.append(x)
        specs.append(all_of(x))
    for x in (east, north):
        ins.append(x)
        specs.append(pl.BlockSpec((nl, across, lat), lambda i, *_: (q, 0, 0)))
    for x in (kmix, water, speeds, precon, rates, pick):
        ins.append(x)
        specs.append(all_of(x))
    out_block = jax.ShapeDtypeStruct((held * nl, cap), jnp.float32)
    shapes = [out_block] * n + [jax.ShapeDtypeStruct((nl, across, lat), jnp.float32)]
    lanes = (cap // LANES + 2) * LANES
    flops = 2 * 12 * rows * rows * lat * nl * (across // ROWS)
    return pl.pallas_call(
        functools.partial(react_kernel, n, nl, q),
        grid_spec=pltpu.PrefetchScalarGridSpec(
            num_scalar_prefetch=3,
            grid=(1,),
            in_specs=specs,
            out_specs=[
                pl.BlockSpec(s.shape, lambda i, *_, k=len(s.shape): (0,) * k) for s in shapes
            ],
            scratch_shapes=[
                pltpu.VMEM((nl * (across // ROWS), rows, lat), jnp.float32),
                pltpu.VMEM((lat // LANES, n * held * nl * across, LANES), jnp.float32),
                pltpu.VMEM((n * held * nl, lanes), jnp.float32),
            ],
        ),
        out_shape=shapes,
        cost_estimate=pl.CostEstimate(
            flops=flops, bytes_accessed=4 * 3 * rows * nl * across * lat // ROWS, transcendentals=0
        ),
        name="react",
    )(me, tiles, shifts, *ins)


def unpack_kernel(n, has_base, *refs):
    _, tile_ref = refs[:2]
    received = refs[2 : 2 + n]
    solute, water, pick, second = refs[2 + n : 6 + n]
    out, slots, spread = refs[6 + n + has_base :]
    held, nl, across, lat = solute.shape
    cap = received[0].shape[1]
    d = pl.program_id(0)
    for k in range(n):

        @pl.when(d == k)
        def _():
            slots[:, :cap] = received[k][...]

    parts = lat // LANES
    for x in range(across):
        for s in range(parts):
            segment = x * parts + s
            tile = pl.multiple_of(tile_ref[segment] * LANES, LANES)
            tail = pl.multiple_of(tile_ref[segment] * LANES + LANES, LANES)
            index = jnp.broadcast_to(pick[segment : segment + 1, :], (ROWS, LANES))
            later = jnp.broadcast_to(second[segment : segment + 1, :], (ROWS, LANES)) > 0
            for g in range(held * nl // ROWS):
                group = slice(g * ROWS, (g + 1) * ROWS)
                a = jnp.take_along_axis(
                    slots[group, pl.ds(tile, LANES)], index, axis=1, mode="promise_in_bounds"
                )
                b = jnp.take_along_axis(
                    slots[group, pl.ds(tail, LANES)], index, axis=1, mode="promise_in_bounds"
                )
                spread[s, pl.ds(g * ROWS * across + x, ROWS, stride=across), :] = jnp.where(
                    later, b, a
                )
    wet = water[...] > 0.5
    for i in range(held):
        for l in range(nl):
            at = (i * nl + l) * across
            for s in range(parts):
                lanes = slice(s * LANES, (s + 1) * LANES)
                out[i, l, :, lanes] = jnp.where(
                    wet[:, lanes], spread[s, at : at + across, :], solute[i, l, :, lanes]
                )


def unpack_chunk(q, parts, me, tiles, received, solute, water, pick, second, base):
    n = len(received)
    held, depth, across, lat = solute.shape
    nl = depth // n // parts
    cap = received[0].shape[1]

    def all_of(x):
        return pl.BlockSpec(x.shape, lambda d, *_: (0,) * x.ndim)

    place = pl.BlockSpec(
        (held, nl, across, lat), lambda d, me, *_: (0, lax.rem(me[0] + d, n) * parts + q, 0, 0)
    )
    specs = [all_of(x) for x in received] + [place, all_of(water), all_of(pick), all_of(second)]
    ins = [*received, solute, water, pick, second]
    aliases = {}
    if base is not None:
        aliases = {2 + len(ins): 0}
        ins.append(base)
        specs.append(pl.BlockSpec(memory_space=pl.ANY))
    return pl.pallas_call(
        functools.partial(unpack_kernel, n, base is not None),
        grid_spec=pltpu.PrefetchScalarGridSpec(
            num_scalar_prefetch=2,
            grid=(n,),
            in_specs=specs,
            out_specs=place,
            scratch_shapes=[
                pltpu.VMEM((held * nl, (cap // LANES + 2) * LANES), jnp.float32),
                pltpu.VMEM((lat // LANES, held * nl * across, LANES), jnp.float32),
            ],
        ),
        out_shape=jax.ShapeDtypeStruct(solute.shape, jnp.float32),
        input_output_aliases=aliases,
        cost_estimate=pl.CostEstimate(
            flops=100 * solute.size, bytes_accessed=12 * solute.size // parts, transcendentals=0
        ),
        name="unpack",
    )(me, tiles, *ins)


def relative(x, me, n, axis):
    x = jnp.flip(x, axis)
    return lax.dynamic_slice_in_dim(jnp.concatenate([x, x], axis), n - 1 - me, n, axis)


def halves_of(x):
    high = lax.reduce_precision(x, 8, 7)
    low = x - high
    return jnp.concatenate([high, high, low], axis=1).astype(jnp.bfloat16)


def plan(held, levels):
    nl = max(levels // 4, ROWS // held)
    parts = levels // nl
    inner = list(range(1, parts - 1))
    return nl, parts, inner + [q for q in range(parts) if q not in inner]


def on_device(
    thermal_state,
    flow_vector,
    vertical_spreading,
    solute_fields,
    linear_exchange_speeds,
    newton_preconditioner,
    absorption_speed,
    water_indicator,
):
    n = lax.axis_size("sec")
    me = lax.axis_index("sec")
    held, depth, across, lat = solute_fields.shape
    tracers = n * held
    levels = depth // n
    nl, parts, order = plan(held, levels)
    me_at = jnp.reshape(me, (1,)).astype(jnp.int32)

    flow_after = shifted(flow_vector[:, :1], "sec", -1)
    before = shifted(
        jnp.concatenate([flow_vector[:, -1:], vertical_spreading[None, -1:]], axis=0), "sec", 1
    )
    thermal_west = around(thermal_state[:, -1:], "col", 1)
    thermal_east = around(thermal_state[:, :1], "col", -1)

    blocks = {}
    for q in range(parts):
        blocks[q] = []
        for d in range(n):
            to = lax.rem(me + d, n)
            block = lax.dynamic_slice_in_dim(solute_fields, to * levels + q * nl, nl, 1)
            blocks[q].append(around(block, "sec", d) if d else block)

    latitude = jnp.pi * (jnp.arange(lat).astype(jnp.float32) + 0.5) / lat - jnp.pi / 2
    rotation = CORIOLIS * jnp.sin(latitude)
    shortwave = jnp.cos(latitude)
    divisor = 1.0 + rotation * rotation

    def turned(flow):
        return ((flow[0] + rotation * flow[1]) / divisor, (flow[1] - rotation * flow[0]) / divisor)

    def mixed(this, below, spread):
        shear = (this[0] - below[0]) ** 2 + (this[1] - below[1]) ** 2
        return 0.5 * spread + 0.5 * shear / (1.0 + shear)

    east, north = turned(flow_vector)
    after = turned(flow_after)
    ahead = turned(before[:2])
    below = tuple(jnp.concatenate([f[1:], g], axis=0) for f, g in zip((east, north), after))
    spreading = mixed((east, north), below, vertical_spreading)
    level_at = me * levels + jnp.arange(levels)
    kmix = jnp.where((level_at < depth - 1)[:, None, None], VERTICAL_MIX * spreading, 0.0)
    ahead_mix = VERTICAL_MIX * mixed(ahead, (east[:1], north[:1]), before[2])
    kmix = jnp.concatenate([jnp.where(me > 0, ahead_mix, 0.0), kmix], axis=0)
    thermal_carried = thermal_state + chemical_change(
        thermal_state,
        jnp.concatenate([thermal_state[:, 1:], thermal_east], axis=1),
        jnp.concatenate([thermal_west, thermal_state[:, :-1]], axis=1),
        east,
        north,
    )

    water = water_indicator.astype(jnp.float32)
    cap = -(-3 * across * lat // 4 // LANES) * LANES
    wet = (water_indicator > 0).astype(jnp.int32).reshape(-1, LANES)
    within = jnp.cumsum(wet, axis=1) - wet
    count = jnp.sum(wet, axis=1)
    offset = jnp.cumsum(count) - count
    tiles = offset // LANES
    shifts = offset % LANES
    slot = within + shifts[:, None]
    lane = jnp.arange(LANES, dtype=jnp.int32)
    hit = (slot % LANES)[:, None, :] == lane[None, :, None]
    gather = jnp.sum(
        jnp.where(hit & (wet > 0)[:, None, :], lane[None, None, :], 0), axis=2, dtype=jnp.int32
    )
    spread_at = slot % LANES
    spread_later = slot // LANES

    speeds = linear_exchange_speeds.reshape(n, held, n, held)
    precon = newton_preconditioner.reshape(n, held, n, held)
    speeds = relative(relative(speeds, me, n, 0), me, n, 2).reshape(tracers, tracers)
    precon = relative(relative(precon, me, n, 0), me, n, 2).reshape(tracers, tracers)
    rates = relative(absorption_speed.reshape(n, held), me, n, 0).reshape(tracers)
    row = jnp.arange(tracers * ROWS, dtype=jnp.int32)
    copy = (row[:, None] // ROWS == jnp.arange(tracers)[None, :]).astype(jnp.float32)
    same = row[:, None] % ROWS == row[None, :] % ROWS

    def widened(x):
        x = jnp.dot(copy, x, precision=lax.Precision.HIGHEST)
        x = jnp.dot(x, copy.T, precision=lax.Precision.HIGHEST)
        return halves_of(jnp.where(same, x, 0.0))

    speeds = widened(speeds)
    precon = widened(precon)
    rates = jnp.dot(
        copy, jnp.broadcast_to(rates[:, None], (tracers, lat)), precision=lax.Precision.HIGHEST
    )

    fields = (east, north, kmix, water, speeds, precon, rates, gather)
    edges = {}
    for q in range(parts):
        level, turn = {0: (0, 1), parts - 1: (nl - 1, n - 1)}.get(q, (None, 0))
        edges[q] = list(chunk_edges(blocks[q], level, turn))
        edges[q][0] = around(edges[q][0], "col", -1)
        edges[q][1] = around(edges[q][1], "col", 1)
    if parts == 1:
        edges[0].append(jnp.concatenate([b[:, -1:] for b in blocks[0][-1:] + blocks[0][:-1]], 0))
    above_all = shifted(edges[0][2], "sec", -1)
    below_all = shifted(edges[parts - 1][-1], "sec", 1)

    pigments = {}
    returned = {}
    for q in order:
        below = (blocks[q - 1], nl - 1) if q > 0 else (below_all, 0)
        above = (blocks[q + 1], 0) if q < parts - 1 else (above_all, 0)
        *packed, pigments[q] = react_chunk(
            q, nl, me_at, tiles, shifts, blocks[q], below, above, edges[q][:2], fields, cap
        )
        returned[q] = []
        for d, x in enumerate(packed):
            returned[q].append(around(x, "sec", -d) if d else x)

    pigment = jnp.concatenate([pigments[q] for q in range(parts)], axis=0)
    square = pigment * pigment
    absorb = WATER_ABSORB + PIGMENT_ABSORB * square / (1.0 + square)
    depth_here = jnp.cumsum(absorb, axis=0)
    total = depth_here[-1]
    over = 0.0
    for d in range(1, n):
        over = over + shifted(total, "sec", d)
    depth_to = over[None] + depth_here
    warming = shortwave * (jnp.exp(-(depth_to - absorb)) - jnp.exp(-depth_to))
    thermal_revised = thermal_carried + CHLOROPHYLL_WARM * water * warming

    solute_revised = None
    for q in order:
        solute_revised = unpack_chunk(
            q, parts, me_at, tiles, returned[q], solute_fields, water, spread_at, spread_later,
            solute_revised,
        )
    return thermal_revised, jnp.stack([east, north]), spreading, solute_revised


def solution(mesh):
    placed = (
        P("sec", "col", None),
        P(None, "sec", "col", None),
        P("sec", "col", None),
        P("sec", None, "col", None),
        P(),
        P(),
        P(),
        P("col", None),
    )
    return jax.shard_map(
        on_device,
        mesh=mesh,
        in_specs=placed,
        out_specs=(
            P("sec", "col", None),
            P(None, "sec", "col", None),
            P("sec", "col", None),
            P("sec", None, "col", None),
        ),
        check_vma=False,
    )
```

```python
import functools

import jax
import jax.numpy as jnp
from jax import lax
from jax.experimental import pallas as pl
from jax.experimental.pallas import tpu as pltpu
from jax.sharding import PartitionSpec as P


NEWTON = 2
CORIOLIS = 0.8
MIXING = 0.1
ADVECTION = 0.2
VERTICAL_MIX = 0.3
WATER_ABSORB = 0.02
PIGMENT_ABSORB = 0.06
CHLOROPHYLL_WARM = 10.0
LANES = 128
ROWS = 8


def shifted(block, axis, distance):
    devices = range(lax.axis_size(axis))
    route = [(i - distance, i) for i in devices if i - distance in devices]
    return lax.ppermute(block, axis, route)


def around(block, axis, distance):
    count = lax.axis_size(axis)
    return lax.ppermute(block, axis, [(i, (i + distance) % count) for i in range(count)])


def chemical_change(center, eastern, western, east_flow, north_flow):
    northern = jnp.concatenate([center[..., 1:], center[..., -1:]], axis=-1)
    southern = jnp.concatenate([center[..., :1], center[..., :-1]], axis=-1)
    laplace = eastern + western + northern + southern - 4.0 * center
    return MIXING * laplace - 0.5 * ADVECTION * (
        east_flow * (eastern - western) + north_flow * (northern - southern)
    )


def edges_kernel(n, level, turn, *refs):
    cur = refs[:n]
    head, tail = refs[n : n + 2]
    held, nl, across, _ = cur[0].shape
    for d in range(n):
        for i in range(held):
            for l in range(nl):
                at = (d * held + i) * nl + l
                head[at : at + 1, :] = cur[d][i, l, 0:1, :]
                tail[at : at + 1, :] = cur[d][i, l, across - 1 : across, :]
    if level is not None:
        for d in range(n):
            refs[n + 2][d * held : (d + 1) * held] = cur[(d + turn) % n][:, level : level + 1]


def chunk_edges(blocks, level, turn):
    n = len(blocks)
    held, nl, across, lat = blocks[0].shape
    shapes = [jax.ShapeDtypeStruct((n * held * nl, lat), jnp.float32)] * 2
    if level is not None:
        shapes.append(jax.ShapeDtypeStruct((n * held, 1, across, lat), jnp.float32))
    return pl.pallas_call(
        functools.partial(edges_kernel, n, level, turn),
        in_specs=[pl.BlockSpec(memory_space=pltpu.VMEM)] * n,
        out_specs=[pl.BlockSpec(memory_space=pltpu.VMEM)] * len(shapes),
        out_shape=shapes,
        cost_estimate=pl.CostEstimate(
            flops=10**8, bytes_accessed=4 * n * blocks[0].size, transcendentals=0
        ),
        name="edges",
    )(*blocks)


def react_kernel(n, nl, q, closing, *refs):
    me_ref, tile_ref, shift_ref = refs[:3]
    cur = refs[3 : 3 + n]
    below = refs[3 + n : 3 + 2 * n]
    above = refs[3 + 2 * n : 3 + 3 * n]
    rest = refs[3 + 3 * n :]
    east_halo, west_halo, east, north, kmix, water, speeds, precon, rates, pick = rest[:10]
    before = rest[10]
    outs = rest[11 : 11 + n]
    absorbs, total = rest[11 + n : 13 + n]
    moved, done, packed = rest[13 + n :]
    held, _, across, lat = cur[0].shape
    tracers = n * held
    halves = across // ROWS

    row_at = lax.broadcasted_iota(jnp.int32, (across, lat), 0)
    lane_at = lax.broadcasted_iota(jnp.int32, (across, lat), 1)
    wet = water[...]
    for l in range(nl):
        u = (0.5 * ADVECTION) * wet * east[l]
        v = (0.5 * ADVECTION) * wet * north[l]
        mix = MIXING * wet
        up = wet * kmix[q * nl + l + 1]
        down = wet * kmix[q * nl + l]
        to_east = mix - u
        to_west = mix + u
        last = lane_at == lat - 1
        first = lane_at == 0
        middle = 1.0 - 4.0 * mix - up - down
        to_north = mix - v
        to_south = mix + v
        middle = middle + jnp.where(last, to_north, 0.0) + jnp.where(first, to_south, 0.0)
        to_north = jnp.where(last, 0.0, to_north)
        to_south = jnp.where(first, 0.0, to_south)
        for d in range(n):
            for i in range(held):
                t = d * held + i
                c = cur[d][i, l]
                lower = cur[d][i, l - 1] if l > 0 else below[d][i, 0]
                upper = cur[d][i, l + 1] if l < nl - 1 else above[d][i, 0]
                at = t * nl + l
                e = jnp.where(
                    row_at == across - 1, east_halo[at : at + 1, :], pltpu.roll(c, across - 1, 0)
                )
                w = jnp.where(row_at == 0, west_halo[at : at + 1, :], pltpu.roll(c, 1, 0))
                value = middle * c + to_east * e + to_west * w
                value = value + to_north * pltpu.roll(c, lat - 1, 1) + to_south * pltpu.roll(c, 1, 1)
                value = value + up * upper + down * lower
                for h in range(halves):
                    moved[l * halves + h, t * ROWS : (t + 1) * ROWS, :] = value[
                        h * ROWS : (h + 1) * ROWS
                    ]

    def product(weights, x):
        high = x.astype(jnp.bfloat16)
        low = (x - high.astype(jnp.float32)).astype(jnp.bfloat16)
        return jnp.dot(
            weights[...],
            jnp.concatenate([high, low, high], axis=0),
            preferred_element_type=jnp.float32,
        )

    def uptake(x):
        square = x * x
        return rates[...] * (square / (1.0 + square))

    def react(j, carry):
        start = moved[j]
        current = start
        for step in range(NEWTON):
            misfit = uptake(current) - product(speeds, current)
            if step > 0:
                misfit = misfit + (current - start)
            current = current - product(precon, misfit)
        l = j // halves
        h = j % halves
        for t in range(tracers):
            at = pl.multiple_of((t * nl + l) * across + h * ROWS, ROWS)
            for s in range(lat // LANES):
                done[s, pl.ds(at, ROWS), :] = current[
                    t * ROWS : (t + 1) * ROWS, s * LANES : (s + 1) * LANES
                ]
        return carry

    lax.fori_loop(0, nl * halves, react, 0)

    me = me_ref[0]
    for s in range(lat // LANES):
        lanes = slice(s * LANES, (s + 1) * LANES)
        column = before[:, lanes]
        for l in range(nl):
            at = pl.multiple_of((me * (held * nl) + l) * across, ROWS)
            pigment = done[s, pl.ds(at, across), :]
            square = pigment * pigment
            absorb = WATER_ABSORB + PIGMENT_ABSORB * square / (1.0 + square)
            absorbs[l, :, lanes] = absorb
            column = column + absorb
        total[:, lanes] = column

    lane = lax.broadcasted_iota(jnp.int32, (ROWS, LANES), 1)
    parts = lat // LANES

    def pack(x, carry):
        for s in range(parts):
            segment = x * parts + s
            tile = pl.multiple_of(tile_ref[segment] * LANES, LANES)
            tail = pl.multiple_of(tile_ref[segment] * LANES + LANES, LANES)
            keep = lane < shift_ref[segment]
            index = jnp.broadcast_to(pick[pl.ds(segment, 1), :], (ROWS, LANES))
            for g in range(tracers * nl // ROWS):
                value = done[s, pl.ds(g * ROWS * across + x, ROWS, stride=across), :]
                value = jnp.take_along_axis(value, index, axis=1, mode="promise_in_bounds")
                here = (slice(g * ROWS, (g + 1) * ROWS), pl.ds(tile, LANES))
                packed[here] = jnp.where(keep, packed[here], value)
                packed[g * ROWS : (g + 1) * ROWS, pl.ds(tail, LANES)] = value
        return carry

    lax.fori_loop(0, across, pack, 0)
    cap = outs[0].shape[1] - (across * lat // (held * nl) if closing else 0)
    for d in range(n):
        outs[d][:, :cap] = packed[d * held * nl : (d + 1) * held * nl, :cap]
        if closing:
            for k in range(across // (held * nl)):
                outs[d][:, cap + k * lat : cap + (k + 1) * lat] = total[
                    k * held * nl : (k + 1) * held * nl, :
                ]


def react_chunk(q, nl, me, tiles, shifts, blocks, below, above, halos, fields, before, cap, closing):
    n = len(blocks)
    held, _, across, lat = blocks[0].shape
    east, north, kmix, water, speeds, precon, rates, pick = fields
    rows = n * held * ROWS
    whole = pl.BlockSpec(memory_space=pltpu.VMEM)

    def level(spec_at):
        return pl.BlockSpec((held, 1, across, lat), lambda i, *_: (0, spec_at, 0, 0))

    def all_of(x):
        return pl.BlockSpec(x.shape, lambda i, *_: (0,) * x.ndim)

    ins = list(blocks)
    specs = [all_of(b) for b in blocks]
    for source, at in (below, above):
        for d in range(n):
            if isinstance(source, list):
                ins.append(source[d])
                specs.append(level(at))
            else:
                ins.append(source)
                specs.append(
                    pl.BlockSpec((held, 1, across, lat), lambda i, *_, d=d: (d, 0, 0, 0))
                )
    for x in halos:
        ins.append(x)
        specs.append(all_of(x))
    for x in (east, north):
        ins.append(x)
        specs.append(pl.BlockSpec((nl, across, lat), lambda i, *_: (q, 0, 0)))
    for x in (kmix, water, speeds, precon, rates, pick, before):
        ins.append(x)
        specs.append(all_of(x))
    wide = cap + (across * lat // (held * nl) if closing else 0)
    shapes = [jax.ShapeDtypeStruct((held * nl, wide), jnp.float32)] * n
    shapes.append(jax.ShapeDtypeStruct((nl, across, lat), jnp.float32))
    shapes.append(jax.ShapeDtypeStruct((across, lat), jnp.float32))
    lanes = (cap // LANES + 2) * LANES
    flops = 2 * 12 * rows * rows * lat * nl * (across // ROWS)
    return pl.pallas_call(
        functools.partial(react_kernel, n, nl, q, closing),
        grid_spec=pltpu.PrefetchScalarGridSpec(
            num_scalar_prefetch=3,
            grid=(1,),
            in_specs=specs,
            out_specs=[
                pl.BlockSpec(s.shape, lambda i, *_, k=len(s.shape): (0,) * k) for s in shapes
            ],
            scratch_shapes=[
                pltpu.VMEM((nl * (across // ROWS), rows, lat), jnp.float32),
                pltpu.VMEM((lat // LANES, n * held * nl * across, LANES), jnp.float32),
                pltpu.VMEM((n * held * nl, lanes), jnp.float32),
            ],
        ),
        out_shape=shapes,
        cost_estimate=pl.CostEstimate(
            flops=flops, bytes_accessed=4 * 3 * rows * nl * across * lat // ROWS, transcendentals=0
        ),
        name="react",
    )(me, tiles, shifts, *ins)


def unpack_kernel(n, cap, has_base, *refs):
    _, tile_ref = refs[:2]
    received = refs[2 : 2 + n]
    solute, water, pick, second = refs[2 + n : 6 + n]
    out, slots, spread = refs[6 + n + has_base :]
    held, nl, across, lat = solute.shape
    d = pl.program_id(0)
    for k in range(n):

        @pl.when(d == k)
        def _():
            slots[:, :cap] = received[k][:, :cap]

    parts = lat // LANES
    for x in range(across):
        for s in range(parts):
            segment = x * parts + s
            tile = pl.multiple_of(tile_ref[segment] * LANES, LANES)
            tail = pl.multiple_of(tile_ref[segment] * LANES + LANES, LANES)
            index = jnp.broadcast_to(pick[segment : segment + 1, :], (ROWS, LANES))
            later = jnp.broadcast_to(second[segment : segment + 1, :], (ROWS, LANES)) > 0
            for g in range(held * nl // ROWS):
                group = slice(g * ROWS, (g + 1) * ROWS)
                a = jnp.take_along_axis(
                    slots[group, pl.ds(tile, LANES)], index, axis=1, mode="promise_in_bounds"
                )
                b = jnp.take_along_axis(
                    slots[group, pl.ds(tail, LANES)], index, axis=1, mode="promise_in_bounds"
                )
                spread[s, pl.ds(g * ROWS * across + x, ROWS, stride=across), :] = jnp.where(
                    later, b, a
                )
    wet = water[...] > 0.5
    for i in range(held):
        for l in range(nl):
            at = (i * nl + l) * across
            for s in range(parts):
                lanes = slice(s * LANES, (s + 1) * LANES)
                out[i, l, :, lanes] = jnp.where(
                    wet[:, lanes], spread[s, at : at + across, :], solute[i, l, :, lanes]
                )


def unpack_chunk(q, parts, me, tiles, received, solute, water, pick, second, base, cap):
    n = len(received)
    held, depth, across, lat = solute.shape
    nl = depth // n // parts

    def all_of(x):
        return pl.BlockSpec(x.shape, lambda d, *_: (0,) * x.ndim)

    place = pl.BlockSpec(
        (held, nl, across, lat), lambda d, me, *_: (0, lax.rem(me[0] + d, n) * parts + q, 0, 0)
    )
    specs = [all_of(x) for x in received] + [place, all_of(water), all_of(pick), all_of(second)]
    ins = [*received, solute, water, pick, second]
    aliases = {}
    if base is not None:
        aliases = {2 + len(ins): 0}
        ins.append(base)
        specs.append(pl.BlockSpec(memory_space=pl.ANY))
    return pl.pallas_call(
        functools.partial(unpack_kernel, n, cap, base is not None),
        grid_spec=pltpu.PrefetchScalarGridSpec(
            num_scalar_prefetch=2,
            grid=(n,),
            in_specs=specs,
            out_specs=place,
            scratch_shapes=[
                pltpu.VMEM((held * nl, (cap // LANES + 2) * LANES), jnp.float32),
                pltpu.VMEM((lat // LANES, held * nl * across, LANES), jnp.float32),
            ],
        ),
        out_shape=jax.ShapeDtypeStruct(solute.shape, jnp.float32),
        input_output_aliases=aliases,
        cost_estimate=pl.CostEstimate(
            flops=100 * solute.size, bytes_accessed=12 * solute.size // parts, transcendentals=0
        ),
        name="unpack",
    )(me, tiles, *ins)


def relative(x, me, n, axis):
    x = jnp.flip(x, axis)
    return lax.dynamic_slice_in_dim(jnp.concatenate([x, x], axis), n - 1 - me, n, axis)


def halves_of(x):
    high = lax.reduce_precision(x, 8, 7)
    low = x - high
    return jnp.concatenate([high, high, low], axis=1).astype(jnp.bfloat16)


def plan(held, levels):
    nl = max(levels // 4, ROWS // held)
    parts = levels // nl
    inner = list(range(1, parts - 1))
    return nl, parts, inner + [q for q in (parts - 1, 0) if q not in inner][: parts - len(inner)]


def on_device(
    thermal_state,
    flow_vector,
    vertical_spreading,
    solute_fields,
    linear_exchange_speeds,
    newton_preconditioner,
    absorption_speed,
    water_indicator,
):
    n = lax.axis_size("sec")
    me = lax.axis_index("sec")
    held, depth, across, lat = solute_fields.shape
    tracers = n * held
    levels = depth // n
    nl, parts, order = plan(held, levels)
    me_at = jnp.reshape(me, (1,)).astype(jnp.int32)

    blocks = {}
    raw = solute_fields
    for q in range(parts):
        sends = []
        for d in range(n):
            to = lax.rem(me + d, n)
            sends.append(lax.dynamic_slice_in_dim(raw, to * levels + q * nl, nl, 1))
        if q == 0:
            raw, *sends = lax.optimization_barrier((raw, *sends))
        blocks[q] = sends[:1]
        for d in range(1, n):
            blocks[q].append(around(sends[d], "sec", d))

    flow_after = shifted(flow_vector[:, :1], "sec", -1)
    before = shifted(
        jnp.concatenate([flow_vector[:, -1:], vertical_spreading[None, -1:]], axis=0), "sec", 1
    )
    thermal_west = around(thermal_state[:, -1:], "col", 1)
    thermal_east = around(thermal_state[:, :1], "col", -1)

    latitude = jnp.pi * (jnp.arange(lat).astype(jnp.float32) + 0.5) / lat - jnp.pi / 2
    rotation = CORIOLIS * jnp.sin(latitude)
    shortwave = jnp.cos(latitude)
    divisor = 1.0 + rotation * rotation

    def turned(flow):
        return ((flow[0] + rotation * flow[1]) / divisor, (flow[1] - rotation * flow[0]) / divisor)

    def mixed(this, below, spread):
        shear = (this[0] - below[0]) ** 2 + (this[1] - below[1]) ** 2
        return 0.5 * spread + 0.5 * shear / (1.0 + shear)

    east, north = turned(flow_vector)
    after = turned(flow_after)
    ahead = turned(before[:2])
    below = tuple(jnp.concatenate([f[1:], g], axis=0) for f, g in zip((east, north), after))
    spreading = mixed((east, north), below, vertical_spreading)
    level_at = me * levels + jnp.arange(levels)
    kmix = jnp.where((level_at < depth - 1)[:, None, None], VERTICAL_MIX * spreading, 0.0)
    ahead_mix = VERTICAL_MIX * mixed(ahead, (east[:1], north[:1]), before[2])
    kmix = jnp.concatenate([jnp.where(me > 0, ahead_mix, 0.0), kmix], axis=0)
    thermal_carried = thermal_state + chemical_change(
        thermal_state,
        jnp.concatenate([thermal_state[:, 1:], thermal_east], axis=1),
        jnp.concatenate([thermal_west, thermal_state[:, :-1]], axis=1),
        east,
        north,
    )

    water = water_indicator.astype(jnp.float32)
    cap = -(-3 * across * lat // 4 // LANES) * LANES
    wet = (water_indicator > 0).astype(jnp.int32).reshape(-1, LANES)
    within = jnp.cumsum(wet, axis=1) - wet
    count = jnp.sum(wet, axis=1)
    offset = jnp.cumsum(count) - count
    tiles = offset // LANES
    shifts = offset % LANES
    slot = within + shifts[:, None]
    lane = jnp.arange(LANES, dtype=jnp.int32)
    hit = (slot % LANES)[:, None, :] == lane[None, :, None]
    gather = jnp.sum(
        jnp.where(hit & (wet > 0)[:, None, :], lane[None, None, :], 0), axis=2, dtype=jnp.int32
    )
    spread_at = slot % LANES
    spread_later = slot // LANES

    speeds = linear_exchange_speeds.reshape(n, held, n, held)
    precon = newton_preconditioner.reshape(n, held, n, held)
    speeds = relative(relative(speeds, me, n, 0), me, n, 2).reshape(tracers, tracers)
    precon = relative(relative(precon, me, n, 0), me, n, 2).reshape(tracers, tracers)
    rates = relative(absorption_speed.reshape(n, held), me, n, 0).reshape(tracers)
    row = jnp.arange(tracers * ROWS, dtype=jnp.int32)
    copy = (row[:, None] // ROWS == jnp.arange(tracers)[None, :]).astype(jnp.float32)
    same = row[:, None] % ROWS == row[None, :] % ROWS

    def widened(x):
        x = jnp.dot(copy, x, precision=lax.Precision.HIGHEST)
        x = jnp.dot(x, copy.T, precision=lax.Precision.HIGHEST)
        return halves_of(jnp.where(same, x, 0.0))

    speeds = widened(speeds)
    precon = widened(precon)
    rates = jnp.dot(
        copy, jnp.broadcast_to(rates[:, None], (tracers, lat)), precision=lax.Precision.HIGHEST
    )

    fields = (east, north, kmix, water, speeds, precon, rates, gather)
    edges = {}
    for q in range(parts):
        level, turn = {0: (0, 1), parts - 1: (nl - 1, n - 1)}.get(q, (None, 0))
        edges[q] = list(chunk_edges(blocks[q], level, turn))
        edges[q][0] = around(edges[q][0], "col", -1)
        edges[q][1] = around(edges[q][1], "col", 1)
    if parts == 1:
        edges[0].append(jnp.concatenate([b[:, -1:] for b in blocks[0][-1:] + blocks[0][:-1]], 0))
    above_all = shifted(edges[0][2], "sec", -1)
    below_all = shifted(edges[parts - 1][-1], "sec", 1)

    absorbs = {}
    returned = {}
    total = jnp.zeros((across, lat), jnp.float32)
    for q in order:
        below = (blocks[q - 1], nl - 1) if q > 0 else (below_all, 0)
        above = (blocks[q + 1], 0) if q < parts - 1 else (above_all, 0)
        *packed, absorbs[q], total = react_chunk(
            q, nl, me_at, tiles, shifts, blocks[q], below, above, edges[q][:2], fields, total,
            cap, q == order[-1],
        )
        returned[q] = []
        for d, x in enumerate(packed):
            returned[q].append(around(x, "sec", -d) if d else x)

    absorb = jnp.concatenate([absorbs[q] for q in range(parts)], axis=0)
    over = 0.0
    for d in range(1, n):
        sums = returned[order[-1]][d][:, cap:]
        sums = [sums[:, k : k + lat] for k in range(0, sums.shape[1], lat)]
        over = over + jnp.where(lax.rem(me + d, n) < me, jnp.concatenate(sums, axis=0), 0.0)
    depth_to = over[None] + jnp.cumsum(absorb, axis=0)
    warming = shortwave * (jnp.exp(-(depth_to - absorb)) - jnp.exp(-depth_to))
    thermal_revised = thermal_carried + CHLOROPHYLL_WARM * water * warming

    solute_revised = None
    for q in order:
        solute_revised = unpack_chunk(
            q, parts, me_at, tiles, returned[q], solute_fields, water, spread_at, spread_later,
            solute_revised, cap,
        )
    return thermal_revised, jnp.stack([east, north]), spreading, solute_revised


def solution(mesh):
    placed = (
        P("sec", "col", None),
        P(None, "sec", "col", None),
        P("sec", "col", None),
        P("sec", None, "col", None),
        P(),
        P(),
        P(),
        P("col", None),
    )
    return jax.shard_map(
        on_device,
        mesh=mesh,
        in_specs=placed,
        out_specs=(
            P("sec", "col", None),
            P(None, "sec", "col", None),
            P("sec", "col", None),
            P("sec", None, "col", None),
        ),
        check_vma=False,
    )
```

```python
import functools

import jax
import jax.numpy as jnp
from jax import lax
from jax.experimental import pallas as pl
from jax.experimental.pallas import tpu as pltpu
from jax.sharding import PartitionSpec as P


NEWTON = 2
CORIOLIS = 0.8
MIXING = 0.1
ADVECTION = 0.2
VERTICAL_MIX = 0.3
WATER_ABSORB = 0.02
PIGMENT_ABSORB = 0.06
CHLOROPHYLL_WARM = 10.0
LANES = 128
ROWS = 8
GAP = 8


def shifted(block, axis, distance):
    devices = range(lax.axis_size(axis))
    route = [(i - distance, i) for i in devices if i - distance in devices]
    return lax.ppermute(block, axis, route)


def around(block, axis, distance):
    count = lax.axis_size(axis)
    return lax.ppermute(block, axis, [(i, (i + distance) % count) for i in range(count)])


def chemical_change(center, eastern, western, east_flow, north_flow):
    northern = jnp.concatenate([center[..., 1:], center[..., -1:]], axis=-1)
    southern = jnp.concatenate([center[..., :1], center[..., :-1]], axis=-1)
    laplace = eastern + western + northern + southern - 4.0 * center
    return MIXING * laplace - 0.5 * ADVECTION * (
        east_flow * (eastern - western) + north_flow * (northern - southern)
    )


def edges_kernel(n, level, turn, *refs):
    cur = refs[:n]
    head, tail = refs[n : n + 2]
    held, nl, across, _ = cur[0].shape
    for d in range(n):
        for i in range(held):
            for l in range(nl):
                at = (d * held + i) * nl + l
                head[at : at + 1, :] = cur[d][i, l, 0:1, :]
                tail[at : at + 1, :] = cur[d][i, l, across - 1 : across, :]
    if level is not None:
        for d in range(n):
            refs[n + 2][d * held : (d + 1) * held] = cur[(d + turn) % n][:, level : level + 1]


def chunk_edges(blocks, level, turn):
    n = len(blocks)
    held, nl, across, lat = blocks[0].shape
    shapes = [jax.ShapeDtypeStruct((n * held * nl, lat), jnp.float32)] * 2
    if level is not None:
        shapes.append(jax.ShapeDtypeStruct((n * held, 1, across, lat), jnp.float32))
    return pl.pallas_call(
        functools.partial(edges_kernel, n, level, turn),
        in_specs=[pl.BlockSpec(memory_space=pltpu.VMEM)] * n,
        out_specs=[pl.BlockSpec(memory_space=pltpu.VMEM)] * len(shapes),
        out_shape=shapes,
        cost_estimate=pl.CostEstimate(
            flops=10**8, bytes_accessed=4 * n * blocks[0].size, transcendentals=0
        ),
        name="edges",
    )(*blocks)


def react_kernel(n, nl, q, closing, *refs):
    me_ref, tile_ref, shift_ref = refs[:3]
    cur = refs[3 : 3 + n]
    below = refs[3 + n : 3 + 2 * n]
    above = refs[3 + 2 * n : 3 + 3 * n]
    rest = refs[3 + 3 * n :]
    east_halo, west_halo, east, north, kmix, water, speeds, precon, rates, pick = rest[:10]
    before = rest[10]
    outs = rest[11 : 11 + n]
    absorbs, total = rest[11 + n : 13 + n]
    moved, done, packed = rest[13 + n :]
    held, _, across, lat = cur[0].shape
    tracers = n * held
    halves = across // ROWS
    pitch = across + GAP

    row_at = lax.broadcasted_iota(jnp.int32, (across, lat), 0)
    lane_at = lax.broadcasted_iota(jnp.int32, (across, lat), 1)
    wet = water[...]
    for l in range(nl):
        u = (0.5 * ADVECTION) * wet * east[l]
        v = (0.5 * ADVECTION) * wet * north[l]
        mix = MIXING * wet
        up = wet * kmix[q * nl + l + 1]
        down = wet * kmix[q * nl + l]
        to_east = mix - u
        to_west = mix + u
        last = lane_at == lat - 1
        first = lane_at == 0
        middle = 1.0 - 4.0 * mix - up - down
        to_north = mix - v
        to_south = mix + v
        middle = middle + jnp.where(last, to_north, 0.0) + jnp.where(first, to_south, 0.0)
        to_north = jnp.where(last, 0.0, to_north)
        to_south = jnp.where(first, 0.0, to_south)
        for d in range(n):
            for i in range(held):
                t = d * held + i
                c = cur[d][i, l]
                lower = cur[d][i, l - 1] if l > 0 else below[d][i, 0]
                upper = cur[d][i, l + 1] if l < nl - 1 else above[d][i, 0]
                at = t * nl + l
                e = jnp.where(
                    row_at == across - 1, east_halo[at : at + 1, :], pltpu.roll(c, across - 1, 0)
                )
                w = jnp.where(row_at == 0, west_halo[at : at + 1, :], pltpu.roll(c, 1, 0))
                value = middle * c + to_east * e + to_west * w
                value = value + to_north * pltpu.roll(c, lat - 1, 1) + to_south * pltpu.roll(c, 1, 1)
                value = value + up * upper + down * lower
                for h in range(halves):
                    moved[l * halves + h, t * ROWS : (t + 1) * ROWS, :] = value[
                        h * ROWS : (h + 1) * ROWS
                    ]

    def product(weights, x):
        high = x.astype(jnp.bfloat16)
        low = (x - high.astype(jnp.float32)).astype(jnp.bfloat16)
        return jnp.dot(
            weights[...],
            jnp.concatenate([high, low, high], axis=0),
            preferred_element_type=jnp.float32,
        )

    def uptake(x):
        square = x * x
        return rates[...] * (square / (1.0 + square))

    def react(j, carry):
        start = moved[j]
        current = start
        for step in range(NEWTON):
            misfit = uptake(current) - product(speeds, current)
            if step > 0:
                misfit = misfit + (current - start)
            current = current - product(precon, misfit)
        l = j // halves
        h = j % halves
        for t in range(tracers):
            at = pl.multiple_of((t * nl + l) * pitch + h * ROWS, ROWS)
            for s in range(lat // LANES):
                done[s, pl.ds(at, ROWS), :] = current[
                    t * ROWS : (t + 1) * ROWS, s * LANES : (s + 1) * LANES
                ]
        return carry

    lax.fori_loop(0, nl * halves, react, 0)

    me = me_ref[0]
    for s in range(lat // LANES):
        lanes = slice(s * LANES, (s + 1) * LANES)
        column = before[:, lanes]
        for l in range(nl):
            at = pl.multiple_of((me * (held * nl) + l) * pitch, ROWS)
            pigment = done[s, pl.ds(at, across), :]
            square = pigment * pigment
            absorb = WATER_ABSORB + PIGMENT_ABSORB * square / (1.0 + square)
            absorbs[l, :, lanes] = absorb
            column = column + absorb
        total[:, lanes] = column

    lane = lax.broadcasted_iota(jnp.int32, (ROWS, LANES), 1)
    parts = lat // LANES

    def pack(x, carry):
        for s in range(parts):
            segment = x * parts + s
            tile = pl.multiple_of(tile_ref[segment] * LANES, LANES)
            tail = pl.multiple_of(tile_ref[segment] * LANES + LANES, LANES)
            keep = lane < shift_ref[segment]
            index = jnp.broadcast_to(pick[pl.ds(segment, 1), :], (ROWS, LANES))
            for g in range(tracers * nl // ROWS):
                value = done[s, pl.ds(g * ROWS * pitch + x, ROWS, stride=pitch), :]
                value = jnp.take_along_axis(value, index, axis=1, mode="promise_in_bounds")
                here = (slice(g * ROWS, (g + 1) * ROWS), pl.ds(tile, LANES))
                packed[here] = jnp.where(keep, packed[here], value)
                packed[g * ROWS : (g + 1) * ROWS, pl.ds(tail, LANES)] = value
        return carry

    lax.fori_loop(0, across, pack, 0)
    cap = outs[0].shape[1] - (across * lat // (held * nl) if closing else 0)
    for d in range(n):
        outs[d][:, :cap] = packed[d * held * nl : (d + 1) * held * nl, :cap]
        if closing:
            for k in range(across // (held * nl)):
                outs[d][:, cap + k * lat : cap + (k + 1) * lat] = total[
                    k * held * nl : (k + 1) * held * nl, :
                ]


def react_chunk(q, nl, me, tiles, shifts, blocks, below, above, halos, fields, before, cap, closing):
    n = len(blocks)
    held, _, across, lat = blocks[0].shape
    east, north, kmix, water, speeds, precon, rates, pick = fields
    rows = n * held * ROWS
    whole = pl.BlockSpec(memory_space=pltpu.VMEM)

    def level(spec_at):
        return pl.BlockSpec((held, 1, across, lat), lambda i, *_: (0, spec_at, 0, 0))

    def all_of(x):
        return pl.BlockSpec(x.shape, lambda i, *_: (0,) * x.ndim)

    ins = list(blocks)
    specs = [all_of(b) for b in blocks]
    for source, at in (below, above):
        for d in range(n):
            if isinstance(source, list):
                ins.append(source[d])
                specs.append(level(at))
            else:
                ins.append(source)
                specs.append(
                    pl.BlockSpec((held, 1, across, lat), lambda i, *_, d=d: (d, 0, 0, 0))
                )
    for x in halos:
        ins.append(x)
        specs.append(all_of(x))
    for x in (east, north):
        ins.append(x)
        specs.append(pl.BlockSpec((nl, across, lat), lambda i, *_: (q, 0, 0)))
    for x in (kmix, water, speeds, precon, rates, pick, before):
        ins.append(x)
        specs.append(all_of(x))
    wide = cap + (across * lat // (held * nl) if closing else 0)
    shapes = [jax.ShapeDtypeStruct((held * nl, wide), jnp.float32)] * n
    shapes.append(jax.ShapeDtypeStruct((nl, across, lat), jnp.float32))
    shapes.append(jax.ShapeDtypeStruct((across, lat), jnp.float32))
    lanes = (cap // LANES + 2) * LANES
    flops = 2 * 12 * rows * rows * lat * nl * (across // ROWS)
    return pl.pallas_call(
        functools.partial(react_kernel, n, nl, q, closing),
        grid_spec=pltpu.PrefetchScalarGridSpec(
            num_scalar_prefetch=3,
            grid=(1,),
            in_specs=specs,
            out_specs=[
                pl.BlockSpec(s.shape, lambda i, *_, k=len(s.shape): (0,) * k) for s in shapes
            ],
            scratch_shapes=[
                pltpu.VMEM((nl * (across // ROWS), rows, lat), jnp.float32),
                pltpu.VMEM((lat // LANES, n * held * nl * (across + GAP), LANES), jnp.float32),
                pltpu.VMEM((n * held * nl, lanes), jnp.float32),
            ],
        ),
        out_shape=shapes,
        cost_estimate=pl.CostEstimate(
            flops=flops, bytes_accessed=4 * 3 * rows * nl * across * lat // ROWS, transcendentals=0
        ),
        name="react",
    )(me, tiles, shifts, *ins)


def unpack_kernel(n, taken, cap, has_base, closing, *refs):
    me_ref, tile_ref = refs[:2]
    received = refs[2 : 2 + len(taken)]
    solute, water, pick, second = refs[2 + len(taken) : 6 + len(taken)]
    rest = refs[6 + len(taken) :]
    if closing:
        totals = rest[: n - 1]
        absorb, sun, carried = rest[n - 1 : n + 2]
        rest = rest[n + 2 :]
    rest = rest[has_base:]
    out, *rest = rest
    if closing:
        warmed, *rest = rest
    slots, spread = rest
    held, nl, across, lat = solute.shape
    pitch = across + GAP
    step = pl.program_id(0)
    for k in range(len(taken)):

        @pl.when(step == k)
        def _():
            slots[:, :cap] = received[k][:, :cap]

    parts = lat // LANES
    for x in range(across):
        for s in range(parts):
            segment = x * parts + s
            tile = pl.multiple_of(tile_ref[segment] * LANES, LANES)
            tail = pl.multiple_of(tile_ref[segment] * LANES + LANES, LANES)
            index = jnp.broadcast_to(pick[segment : segment + 1, :], (ROWS, LANES))
            later = jnp.broadcast_to(second[segment : segment + 1, :], (ROWS, LANES)) > 0
            for g in range(held * nl // ROWS):
                group = slice(g * ROWS, (g + 1) * ROWS)
                a = jnp.take_along_axis(
                    slots[group, pl.ds(tile, LANES)], index, axis=1, mode="promise_in_bounds"
                )
                b = jnp.take_along_axis(
                    slots[group, pl.ds(tail, LANES)], index, axis=1, mode="promise_in_bounds"
                )
                spread[s, pl.ds(g * ROWS * pitch + x, ROWS, stride=pitch), :] = jnp.where(
                    later, b, a
                )
    wet = water[...] > 0.5
    for i in range(held):
        for l in range(nl):
            at = (i * nl + l) * pitch
            for s in range(parts):
                lanes = slice(s * LANES, (s + 1) * LANES)
                out[i, l, :, lanes] = jnp.where(
                    wet[:, lanes], spread[s, at : at + across, :], solute[i, l, :, lanes]
                )
    if closing:

        @pl.when(step == 0)
        def _():
            size = held * nl
            here = me_ref[0]
            for k in range(across // size):
                lane = slice(k * lat, (k + 1) * lat)
                row = slice(k * size, (k + 1) * size)
                over = jnp.zeros((size, lat), jnp.float32)
                for d in range(1, n):
                    above = lax.rem(here + d, n) < here
                    over = over + jnp.where(above, totals[d - 1][:, lane], 0.0)
                light = sun[...] * (CHLOROPHYLL_WARM * water[row, :])
                coming = jnp.exp(-over)
                for l in range(absorb.shape[0]):
                    over = over + absorb[l, row, :]
                    left = jnp.exp(-over)
                    warmed[l, row, :] = carried[l, row, :] + light * (coming - left)
                    coming = left


def unpack_chunk(
    q, parts, me, tiles, returned, taken, solute, water, pick, second, base, cap, heat=None
):
    n = len(returned)
    held, depth, across, lat = solute.shape
    nl = depth // n // parts
    received = [returned[d] for d in taken]

    def all_of(x):
        return pl.BlockSpec(x.shape, lambda i, *_: (0,) * x.ndim)

    def place_at(i, me, *_):
        d = sum(jnp.where(i == k, d, 0) for k, d in enumerate(taken))
        return 0, lax.rem(me[0] + d, n) * parts + q, 0, 0

    place = pl.BlockSpec((held, nl, across, lat), place_at)
    ins = [*received, solute, water, pick, second]
    specs = [all_of(x) for x in received] + [place, all_of(water), all_of(pick), all_of(second)]
    shapes = [jax.ShapeDtypeStruct(solute.shape, jnp.float32)]
    outs = [place]
    if heat is not None:
        width = across * lat // (held * nl)
        for d in range(1, n):
            ins.append(returned[d])
            specs.append(pl.BlockSpec((held * nl, width), lambda i, *_: (0, cap // width)))
        for x in heat:
            ins.append(x)
            specs.append(all_of(x))
        shapes.append(jax.ShapeDtypeStruct(heat[-1].shape, jnp.float32))
        outs.append(all_of(heat[-1]))
    aliases = {}
    if base is not None:
        aliases = {2 + len(ins): 0}
        ins.append(base)
        specs.append(pl.BlockSpec(memory_space=pl.ANY))
    return pl.pallas_call(
        functools.partial(
            unpack_kernel, n, taken, cap, base is not None, heat is not None
        ),
        grid_spec=pltpu.PrefetchScalarGridSpec(
            num_scalar_prefetch=2,
            grid=(len(taken),),
            in_specs=specs,
            out_specs=outs,
            scratch_shapes=[
                pltpu.VMEM((held * nl, (cap // LANES + 2) * LANES), jnp.float32),
                pltpu.VMEM((lat // LANES, held * nl * (across + GAP), LANES), jnp.float32),
            ],
        ),
        out_shape=shapes,
        input_output_aliases=aliases,
        cost_estimate=pl.CostEstimate(
            flops=100 * solute.size, bytes_accessed=12 * solute.size // parts, transcendentals=0
        ),
        name="unpack",
    )(me, tiles, *ins)


def relative(x, me, n, axis):
    x = jnp.flip(x, axis)
    return lax.dynamic_slice_in_dim(jnp.concatenate([x, x], axis), n - 1 - me, n, axis)


def halves_of(x):
    high = lax.reduce_precision(x, 8, 7)
    low = x - high
    return jnp.concatenate([high, high, low], axis=1).astype(jnp.bfloat16)


def plan(held, levels):
    nl = max(levels // 4, ROWS // held)
    parts = levels // nl
    inner = list(range(1, parts - 1))
    return nl, parts, inner + [q for q in (parts - 1, 0) if q not in inner][: parts - len(inner)]


def reach(n):
    return sorted(range(1, n), key=lambda d: (-min(d, n - d), d))


def on_device(
    thermal_state,
    flow_vector,
    vertical_spreading,
    solute_fields,
    linear_exchange_speeds,
    newton_preconditioner,
    absorption_speed,
    water_indicator,
):
    n = lax.axis_size("sec")
    me = lax.axis_index("sec")
    held, depth, across, lat = solute_fields.shape
    tracers = n * held
    levels = depth // n
    nl, parts, order = plan(held, levels)
    me_at = jnp.reshape(me, (1,)).astype(jnp.int32)

    blocks = {}
    raw = solute_fields
    for q in range(parts):
        sends = {}
        for d in reach(n):
            to = lax.rem(me + d, n)
            sends[d] = lax.dynamic_slice_in_dim(raw, to * levels + q * nl, nl, 1)
        if q == 0:
            raw, sends = lax.optimization_barrier((raw, sends))
        blocks[q] = [lax.dynamic_slice_in_dim(raw, me * levels + q * nl, nl, 1)]
        for d in range(1, n):
            blocks[q].append(around(sends[d], "sec", d))

    flow_after = shifted(flow_vector[:, :1], "sec", -1)
    before = shifted(
        jnp.concatenate([flow_vector[:, -1:], vertical_spreading[None, -1:]], axis=0), "sec", 1
    )
    thermal_west = around(thermal_state[:, -1:], "col", 1)
    thermal_east = around(thermal_state[:, :1], "col", -1)

    latitude = jnp.pi * (jnp.arange(lat).astype(jnp.float32) + 0.5) / lat - jnp.pi / 2
    rotation = CORIOLIS * jnp.sin(latitude)
    shortwave = jnp.cos(latitude)
    divisor = 1.0 + rotation * rotation

    def turned(flow):
        return ((flow[0] + rotation * flow[1]) / divisor, (flow[1] - rotation * flow[0]) / divisor)

    def mixed(this, below, spread):
        shear = (this[0] - below[0]) ** 2 + (this[1] - below[1]) ** 2
        return 0.5 * spread + 0.5 * shear / (1.0 + shear)

    east, north = turned(flow_vector)
    after = turned(flow_after)
    ahead = turned(before[:2])
    below = tuple(jnp.concatenate([f[1:], g], axis=0) for f, g in zip((east, north), after))
    spreading = mixed((east, north), below, vertical_spreading)
    level_at = me * levels + jnp.arange(levels)
    kmix = jnp.where((level_at < depth - 1)[:, None, None], VERTICAL_MIX * spreading, 0.0)
    ahead_mix = VERTICAL_MIX * mixed(ahead, (east[:1], north[:1]), before[2])
    kmix = jnp.concatenate([jnp.where(me > 0, ahead_mix, 0.0), kmix], axis=0)
    thermal_carried = thermal_state + chemical_change(
        thermal_state,
        jnp.concatenate([thermal_state[:, 1:], thermal_east], axis=1),
        jnp.concatenate([thermal_west, thermal_state[:, :-1]], axis=1),
        east,
        north,
    )

    water = water_indicator.astype(jnp.float32)
    cap = -(-3 * across * lat // 4 // LANES) * LANES
    wet = (water_indicator > 0).astype(jnp.int32).reshape(-1, LANES)
    within = jnp.cumsum(wet, axis=1) - wet
    count = jnp.sum(wet, axis=1)
    offset = jnp.cumsum(count) - count
    tiles = offset // LANES
    shifts = offset % LANES
    slot = within + shifts[:, None]
    lane = jnp.arange(LANES, dtype=jnp.int32)
    hit = (slot % LANES)[:, None, :] == lane[None, :, None]
    gather = jnp.sum(
        jnp.where(hit & (wet > 0)[:, None, :], lane[None, None, :], 0), axis=2, dtype=jnp.int32
    )
    spread_at = slot % LANES
    spread_later = slot // LANES

    speeds = linear_exchange_speeds.reshape(n, held, n, held)
    precon = newton_preconditioner.reshape(n, held, n, held)
    speeds = relative(relative(speeds, me, n, 0), me, n, 2).reshape(tracers, tracers)
    precon = relative(relative(precon, me, n, 0), me, n, 2).reshape(tracers, tracers)
    rates = relative(absorption_speed.reshape(n, held), me, n, 0).reshape(tracers)
    row = jnp.arange(tracers * ROWS, dtype=jnp.int32)
    copy = (row[:, None] // ROWS == jnp.arange(tracers)[None, :]).astype(jnp.float32)
    same = row[:, None] % ROWS == row[None, :] % ROWS

    def widened(x):
        x = jnp.dot(copy, x, precision=lax.Precision.HIGHEST)
        x = jnp.dot(x, copy.T, precision=lax.Precision.HIGHEST)
        return halves_of(jnp.where(same, x, 0.0))

    speeds = widened(speeds)
    precon = widened(precon)
    rates = jnp.dot(
        copy, jnp.broadcast_to(rates[:, None], (tracers, lat)), precision=lax.Precision.HIGHEST
    )

    fields = (east, north, kmix, water, speeds, precon, rates, gather)
    edges = {}
    for q in range(parts):
        level, turn = {0: (0, 1), parts - 1: (nl - 1, n - 1)}.get(q, (None, 0))
        edges[q] = list(chunk_edges(blocks[q], level, turn))
        edges[q][0] = around(edges[q][0], "col", -1)
        edges[q][1] = around(edges[q][1], "col", 1)
    if parts == 1:
        edges[0].append(jnp.concatenate([b[:, -1:] for b in blocks[0][-1:] + blocks[0][:-1]], 0))
    above_all = shifted(edges[0][2], "sec", -1)
    below_all = shifted(edges[parts - 1][-1], "sec", 1)

    absorbs = {}
    returned = {}
    total = jnp.zeros((across, lat), jnp.float32)
    for q in order:
        below = (blocks[q - 1], nl - 1) if q > 0 else (below_all, 0)
        above = (blocks[q + 1], 0) if q < parts - 1 else (above_all, 0)
        *packed, absorbs[q], total = react_chunk(
            q, nl, me_at, tiles, shifts, blocks[q], below, above, edges[q][:2], fields, total,
            cap, q == order[-1],
        )
        returned[q] = []
        for d, x in enumerate(packed):
            returned[q].append(around(x, "sec", -d) if d else x)

    absorb = jnp.concatenate([absorbs[q] for q in range(parts)], axis=0)
    sun = shortwave[None, :]

    calls = [(q, tuple(range(n))) for q in order[:-1]]
    far = [0, *reach(n)]
    calls += [(order[-1], tuple(far[: n // 2])), (order[-1], tuple(far[n // 2 :]))]
    solute_revised = None
    for k, (q, taken) in enumerate(calls):
        heat = (absorb, sun, thermal_carried) if k == len(calls) - 1 else None
        solute_revised, *thermal_revised = unpack_chunk(
            q, parts, me_at, tiles, returned[q], taken, solute_fields, water, spread_at,
            spread_later, solute_revised, cap, heat,
        )
    return thermal_revised[0], jnp.stack([east, north]), spreading, solute_revised


def solution(mesh):
    placed = (
        P("sec", "col", None),
        P(None, "sec", "col", None),
        P("sec", "col", None),
        P("sec", None, "col", None),
        P(),
        P(),
        P(),
        P("col", None),
    )
    return jax.shard_map(
        on_device,
        mesh=mesh,
        in_specs=placed,
        out_specs=(
            P("sec", "col", None),
            P(None, "sec", "col", None),
            P("sec", "col", None),
            P("sec", None, "col", None),
        ),
        check_vma=False,
    )
```

```python
import functools

import jax
import jax.numpy as jnp
from jax import lax
from jax.experimental import pallas as pl
from jax.experimental.pallas import tpu as pltpu
from jax.sharding import PartitionSpec as P


NEWTON = 2
CORIOLIS = 0.8
MIXING = 0.1
ADVECTION = 0.2
VERTICAL_MIX = 0.3
WATER_ABSORB = 0.02
PIGMENT_ABSORB = 0.06
CHLOROPHYLL_WARM = 10.0
LANES = 128
ROWS = 8
GAP = 8


def shifted(block, axis, distance):
    devices = range(lax.axis_size(axis))
    route = [(i - distance, i) for i in devices if i - distance in devices]
    return lax.ppermute(block, axis, route)


def around(block, axis, distance):
    count = lax.axis_size(axis)
    return lax.ppermute(block, axis, [(i, (i + distance) % count) for i in range(count)])


def chemical_change(center, eastern, western, east_flow, north_flow):
    northern = jnp.concatenate([center[..., 1:], center[..., -1:]], axis=-1)
    southern = jnp.concatenate([center[..., :1], center[..., :-1]], axis=-1)
    laplace = eastern + western + northern + southern - 4.0 * center
    return MIXING * laplace - 0.5 * ADVECTION * (
        east_flow * (eastern - western) + north_flow * (northern - southern)
    )


def edges_kernel(n, level, turn, *refs):
    cur = refs[:n]
    head, tail = refs[n : n + 2]
    held, nl, across, _ = cur[0].shape
    for d in range(n):
        for i in range(held):
            for l in range(nl):
                at = (d * held + i) * nl + l
                head[at : at + 1, :] = cur[d][i, l, 0:1, :]
                tail[at : at + 1, :] = cur[d][i, l, across - 1 : across, :]
    if level is not None:
        for d in range(n):
            refs[n + 2][d * held : (d + 1) * held] = cur[(d + turn) % n][:, level : level + 1]


def chunk_edges(blocks, level, turn):
    n = len(blocks)
    held, nl, across, lat = blocks[0].shape
    shapes = [jax.ShapeDtypeStruct((n * held * nl, lat), jnp.float32)] * 2
    if level is not None:
        shapes.append(jax.ShapeDtypeStruct((n * held, 1, across, lat), jnp.float32))
    return pl.pallas_call(
        functools.partial(edges_kernel, n, level, turn),
        in_specs=[pl.BlockSpec(memory_space=pltpu.VMEM)] * n,
        out_specs=[pl.BlockSpec(memory_space=pltpu.VMEM)] * len(shapes),
        out_shape=shapes,
        cost_estimate=pl.CostEstimate(
            flops=10**8, bytes_accessed=4 * n * blocks[0].size, transcendentals=0
        ),
        name="edges",
    )(*blocks)


def react_kernel(n, nl, q, closing, *refs):
    me_ref, tile_ref, shift_ref = refs[:3]
    cur = refs[3 : 3 + n]
    below = refs[3 + n : 3 + 2 * n]
    above = refs[3 + 2 * n : 3 + 3 * n]
    rest = refs[3 + 3 * n :]
    east_halo, west_halo, east, north, kmix, water, speeds, precon, rates, pick = rest[:10]
    before = rest[10]
    outs = rest[11 : 11 + n]
    absorbs, total = rest[11 + n : 13 + n]
    moved, done, packed = rest[13 + n :]
    held, _, across, lat = cur[0].shape
    tracers = n * held
    halves = across // ROWS
    pitch = across + GAP

    row_at = lax.broadcasted_iota(jnp.int32, (across, lat), 0)
    lane_at = lax.broadcasted_iota(jnp.int32, (across, lat), 1)
    wet = water[...]
    for l in range(nl):
        u = (0.5 * ADVECTION) * wet * east[l]
        v = (0.5 * ADVECTION) * wet * north[l]
        mix = MIXING * wet
        up = wet * kmix[q * nl + l + 1]
        down = wet * kmix[q * nl + l]
        to_east = mix - u
        to_west = mix + u
        last = lane_at == lat - 1
        first = lane_at == 0
        middle = 1.0 - 4.0 * mix - up - down
        to_north = mix - v
        to_south = mix + v
        middle = middle + jnp.where(last, to_north, 0.0) + jnp.where(first, to_south, 0.0)
        to_north = jnp.where(last, 0.0, to_north)
        to_south = jnp.where(first, 0.0, to_south)
        for d in range(n):
            for i in range(held):
                t = d * held + i
                c = cur[d][i, l]
                lower = cur[d][i, l - 1] if l > 0 else below[d][i, 0]
                upper = cur[d][i, l + 1] if l < nl - 1 else above[d][i, 0]
                at = t * nl + l
                e = jnp.where(
                    row_at == across - 1, east_halo[at : at + 1, :], pltpu.roll(c, across - 1, 0)
                )
                w = jnp.where(row_at == 0, west_halo[at : at + 1, :], pltpu.roll(c, 1, 0))
                value = middle * c + to_east * e + to_west * w
                value = value + to_north * pltpu.roll(c, lat - 1, 1) + to_south * pltpu.roll(c, 1, 1)
                value = value + up * upper + down * lower
                for h in range(halves):
                    moved[l * halves + h, t * ROWS : (t + 1) * ROWS, :] = value[
                        h * ROWS : (h + 1) * ROWS
                    ]

    def product(weights, x):
        high = x.astype(jnp.bfloat16)
        low = (x - high.astype(jnp.float32)).astype(jnp.bfloat16)
        return jnp.dot(
            weights[...],
            jnp.concatenate([high, low, high], axis=0),
            preferred_element_type=jnp.float32,
        )

    def uptake(x):
        square = x * x
        return rates[...] * (square / (1.0 + square))

    def react(j, carry):
        start = moved[j]
        current = start
        for step in range(NEWTON):
            misfit = uptake(current) - product(speeds, current)
            if step > 0:
                misfit = misfit + (current - start)
            current = current - product(precon, misfit)
        l = j // halves
        h = j % halves
        for t in range(tracers):
            at = pl.multiple_of((t * nl + l) * pitch + h * ROWS, ROWS)
            for s in range(lat // LANES):
                done[s, pl.ds(at, ROWS), :] = current[
                    t * ROWS : (t + 1) * ROWS, s * LANES : (s + 1) * LANES
                ]
        return carry

    lax.fori_loop(0, nl * halves, react, 0)

    me = me_ref[0]
    for s in range(lat // LANES):
        lanes = slice(s * LANES, (s + 1) * LANES)
        column = before[:, lanes]
        for l in range(nl):
            at = pl.multiple_of((me * (held * nl) + l) * pitch, ROWS)
            pigment = done[s, pl.ds(at, across), :]
            square = pigment * pigment
            absorb = WATER_ABSORB + PIGMENT_ABSORB * square / (1.0 + square)
            absorbs[l, :, lanes] = absorb
            column = column + absorb
        total[:, lanes] = column

    lane = lax.broadcasted_iota(jnp.int32, (ROWS, LANES), 1)
    parts = lat // LANES

    def pack(x, carry):
        for s in range(parts):
            segment = x * parts + s
            tile = pl.multiple_of(tile_ref[segment] * LANES, LANES)
            tail = pl.multiple_of(tile_ref[segment] * LANES + LANES, LANES)
            keep = lane < shift_ref[segment]
            index = jnp.broadcast_to(pick[pl.ds(segment, 1), :], (ROWS, LANES))
            for g in range(tracers * nl // ROWS):
                value = done[s, pl.ds(g * ROWS * pitch + x, ROWS, stride=pitch), :]
                value = jnp.take_along_axis(value, index, axis=1, mode="promise_in_bounds")
                here = (slice(g * ROWS, (g + 1) * ROWS), pl.ds(tile, LANES))
                packed[here] = jnp.where(keep, packed[here], value)
                packed[g * ROWS : (g + 1) * ROWS, pl.ds(tail, LANES)] = value
        return carry

    lax.fori_loop(0, across, pack, 0)
    cap = outs[0].shape[1] - (across * lat // (held * nl) if closing else 0)
    for d in range(n):
        outs[d][:, :cap] = packed[d * held * nl : (d + 1) * held * nl, :cap]
        if closing:
            for k in range(across // (held * nl)):
                outs[d][:, cap + k * lat : cap + (k + 1) * lat] = total[
                    k * held * nl : (k + 1) * held * nl, :
                ]


def react_chunk(q, nl, me, tiles, shifts, blocks, below, above, halos, fields, before, cap, closing):
    n = len(blocks)
    held, _, across, lat = blocks[0].shape
    east, north, kmix, water, speeds, precon, rates, pick = fields
    rows = n * held * ROWS
    whole = pl.BlockSpec(memory_space=pltpu.VMEM)

    def level(spec_at):
        return pl.BlockSpec((held, 1, across, lat), lambda i, *_: (0, spec_at, 0, 0))

    def all_of(x):
        return pl.BlockSpec(x.shape, lambda i, *_: (0,) * x.ndim)

    ins = list(blocks)
    specs = [all_of(b) for b in blocks]
    for source, at in (below, above):
        for d in range(n):
            if isinstance(source, list):
                ins.append(source[d])
                specs.append(level(at))
            else:
                ins.append(source)
                specs.append(
                    pl.BlockSpec((held, 1, across, lat), lambda i, *_, d=d: (d, 0, 0, 0))
                )
    for x in halos:
        ins.append(x)
        specs.append(all_of(x))
    for x in (east, north):
        ins.append(x)
        specs.append(pl.BlockSpec((nl, across, lat), lambda i, *_: (q, 0, 0)))
    for x in (kmix, water, speeds, precon, rates, pick, before):
        ins.append(x)
        specs.append(all_of(x))
    wide = cap + (across * lat // (held * nl) if closing else 0)
    shapes = [jax.ShapeDtypeStruct((held * nl, wide), jnp.float32)] * n
    shapes.append(jax.ShapeDtypeStruct((nl, across, lat), jnp.float32))
    shapes.append(jax.ShapeDtypeStruct((across, lat), jnp.float32))
    lanes = (cap // LANES + 2) * LANES
    flops = 2 * 12 * rows * rows * lat * nl * (across // ROWS)
    return pl.pallas_call(
        functools.partial(react_kernel, n, nl, q, closing),
        grid_spec=pltpu.PrefetchScalarGridSpec(
            num_scalar_prefetch=3,
            grid=(1,),
            in_specs=specs,
            out_specs=[
                pl.BlockSpec(s.shape, lambda i, *_, k=len(s.shape): (0,) * k) for s in shapes
            ],
            scratch_shapes=[
                pltpu.VMEM((nl * (across // ROWS), rows, lat), jnp.float32),
                pltpu.VMEM((lat // LANES, n * held * nl * (across + GAP), LANES), jnp.float32),
                pltpu.VMEM((n * held * nl, lanes), jnp.float32),
            ],
        ),
        out_shape=shapes,
        cost_estimate=pl.CostEstimate(
            flops=flops, bytes_accessed=4 * 3 * rows * nl * across * lat // ROWS, transcendentals=0
        ),
        name="react",
    )(me, tiles, shifts, *ins)


def unpack_kernel(n, taken, nl, cap, at_level, has_base, closing, *refs):
    me_ref, tile_ref = refs[:2]
    received = refs[2 : 2 + len(taken)]
    solute, water, pick, second = refs[2 + len(taken) : 6 + len(taken)]
    rest = refs[6 + len(taken) :]
    if closing:
        totals = rest[: n - 1]
        absorb, sun, carried = rest[n - 1 : n + 2]
        rest = rest[n + 2 :]
    rest = rest[has_base:]
    out, *rest = rest
    if closing:
        warmed, *rest = rest
    slots, water_in, spread, sems = rest
    held, depth, across, lat = solute.shape
    levels = depth // n
    pitch = across + GAP
    here = me_ref[0]
    count = len(taken)

    def place(k):
        d = sum(jnp.where(k == j, d, 0) for j, d in enumerate(taken))
        return pl.ds(lax.rem(here + d, n) * levels + at_level, nl)

    def packed_in(k, source):
        return pltpu.make_async_copy(
            source.at[:, pl.ds(0, cap)], slots.at[k, :, pl.ds(0, cap)], sems.at[0, k]
        )

    def block_in(k):
        return pltpu.make_async_copy(solute.at[:, place(k)], water_in.at[k], sems.at[1, k])

    def block_out(k):
        return pltpu.make_async_copy(water_in.at[k], out.at[:, place(k)], sems.at[2, k])

    for k in range(count):
        packed_in(k, received[k]).start()
        block_in(k).start()
    wet = water[...] > 0.5

    def unpack(k, carry):
        packed_in(k, received[0]).wait()
        block_in(k).wait()
        spread_block(k, tile_ref, pick, second, slots, spread, held * nl, across, lat)
        for i in range(held):
            for l in range(nl):
                at = (i * nl + l) * pitch
                for s in range(lat // LANES):
                    lanes = slice(s * LANES, (s + 1) * LANES)
                    water_in[k, i, l, :, lanes] = jnp.where(
                        wet[:, lanes], spread[s, at : at + across, :], water_in[k, i, l, :, lanes]
                    )
        block_out(k).start()
        return carry

    lax.fori_loop(0, count, unpack, 0)
    if closing:
        size = held * nl
        for k in range(across // size):
            lane = slice(k * lat, (k + 1) * lat)
            row = slice(k * size, (k + 1) * size)
            over = jnp.zeros((size, lat), jnp.float32)
            for d in range(1, n):
                above = lax.rem(here + d, n) < here
                over = over + jnp.where(above, totals[d - 1][:, lane], 0.0)
            light = sun[...] * (CHLOROPHYLL_WARM * water[row, :])
            coming = jnp.exp(-over)
            for l in range(absorb.shape[0]):
                over = over + absorb[l, row, :]
                left = jnp.exp(-over)
                warmed[l, row, :] = carried[l, row, :] + light * (coming - left)
                coming = left
    for k in range(count):
        block_out(k).wait()


def spread_block(k, tile_ref, pick, second, slots, spread, rows, across, lat):
    pitch = across + GAP
    parts = lat // LANES
    for x in range(across):
        for s in range(parts):
            segment = x * parts + s
            tile = pl.multiple_of(tile_ref[segment] * LANES, LANES)
            tail = pl.multiple_of(tile_ref[segment] * LANES + LANES, LANES)
            index = jnp.broadcast_to(pick[segment : segment + 1, :], (ROWS, LANES))
            later = jnp.broadcast_to(second[segment : segment + 1, :], (ROWS, LANES)) > 0
            for g in range(rows // ROWS):
                group = slice(g * ROWS, (g + 1) * ROWS)
                a = jnp.take_along_axis(
                    slots[k, group, pl.ds(tile, LANES)], index, axis=1, mode="promise_in_bounds"
                )
                b = jnp.take_along_axis(
                    slots[k, group, pl.ds(tail, LANES)], index, axis=1, mode="promise_in_bounds"
                )
                spread[s, pl.ds(g * ROWS * pitch + x, ROWS, stride=pitch), :] = jnp.where(
                    later, b, a
                )


def unpack_chunk(
    q, parts, me, tiles, returned, taken, solute, water, pick, second, base, cap, heat=None
):
    n = len(returned)
    held, depth, across, lat = solute.shape
    nl = depth // n // parts
    received = [returned[d] for d in taken]

    def all_of(x):
        return pl.BlockSpec(x.shape, lambda i, *_: (0,) * x.ndim)

    apart = pl.BlockSpec(memory_space=pl.ANY)
    ins = [*received, solute, water, pick, second]
    specs = [apart] * (len(taken) + 1) + [all_of(water), all_of(pick), all_of(second)]
    shapes = [jax.ShapeDtypeStruct(solute.shape, jnp.float32)]
    outs = [apart]
    if heat is not None:
        width = across * lat // (held * nl)
        for d in range(1, n):
            ins.append(returned[d])
            specs.append(pl.BlockSpec((held * nl, width), lambda i, *_: (0, cap // width)))
        for x in heat:
            ins.append(x)
            specs.append(all_of(x))
        shapes.append(jax.ShapeDtypeStruct(heat[-1].shape, jnp.float32))
        outs.append(all_of(heat[-1]))
    aliases = {}
    if base is not None:
        aliases = {2 + len(ins): 0}
        ins.append(base)
        specs.append(pl.BlockSpec(memory_space=pl.ANY))
    return pl.pallas_call(
        functools.partial(
            unpack_kernel, n, taken, nl, cap, q * nl, base is not None, heat is not None
        ),
        grid_spec=pltpu.PrefetchScalarGridSpec(
            num_scalar_prefetch=2,
            grid=(1,),
            in_specs=specs,
            out_specs=outs,
            scratch_shapes=[
                pltpu.VMEM((len(taken), held * nl, (cap // LANES + 2) * LANES), jnp.float32),
                pltpu.VMEM((len(taken), held, nl, across, lat), jnp.float32),
                pltpu.VMEM((lat // LANES, held * nl * (across + GAP), LANES), jnp.float32),
                pltpu.SemaphoreType.DMA((3, len(taken))),
            ],
        ),
        out_shape=shapes,
        input_output_aliases=aliases,
        cost_estimate=pl.CostEstimate(
            flops=100 * solute.size, bytes_accessed=12 * solute.size // parts, transcendentals=0
        ),
        name="unpack",
    )(me, tiles, *ins)


def relative(x, me, n, axis):
    x = jnp.flip(x, axis)
    return lax.dynamic_slice_in_dim(jnp.concatenate([x, x], axis), n - 1 - me, n, axis)


def halves_of(x):
    high = lax.reduce_precision(x, 8, 7)
    low = x - high
    return jnp.concatenate([high, high, low], axis=1).astype(jnp.bfloat16)


def plan(held, levels):
    nl = max(levels // 4, ROWS // held)
    parts = levels // nl
    inner = list(range(1, parts - 1))
    return nl, parts, inner + [q for q in (parts - 1, 0) if q not in inner][: parts - len(inner)]


def reach(n):
    return sorted(range(1, n), key=lambda d: (-min(d, n - d), d))


def on_device(
    thermal_state,
    flow_vector,
    vertical_spreading,
    solute_fields,
    linear_exchange_speeds,
    newton_preconditioner,
    absorption_speed,
    water_indicator,
):
    n = lax.axis_size("sec")
    me = lax.axis_index("sec")
    held, depth, across, lat = solute_fields.shape
    tracers = n * held
    levels = depth // n
    nl, parts, order = plan(held, levels)
    me_at = jnp.reshape(me, (1,)).astype(jnp.int32)

    blocks = {}
    raw = solute_fields
    for q in range(parts):
        sends = {}
        for d in reach(n):
            to = lax.rem(me + d, n)
            sends[d] = lax.dynamic_slice_in_dim(raw, to * levels + q * nl, nl, 1)
            if q == 0 and d in reach(n)[:: n - 2]:
                raw, sends = lax.optimization_barrier((raw, sends))
        blocks[q] = [lax.dynamic_slice_in_dim(raw, me * levels + q * nl, nl, 1)]
        for d in range(1, n):
            blocks[q].append(around(sends[d], "sec", d))

    flow_after = shifted(flow_vector[:, :1], "sec", -1)
    before = shifted(
        jnp.concatenate([flow_vector[:, -1:], vertical_spreading[None, -1:]], axis=0), "sec", 1
    )
    thermal_west = around(thermal_state[:, -1:], "col", 1)
    thermal_east = around(thermal_state[:, :1], "col", -1)

    latitude = jnp.pi * (jnp.arange(lat).astype(jnp.float32) + 0.5) / lat - jnp.pi / 2
    rotation = CORIOLIS * jnp.sin(latitude)
    shortwave = jnp.cos(latitude)
    divisor = 1.0 + rotation * rotation

    def turned(flow):
        return ((flow[0] + rotation * flow[1]) / divisor, (flow[1] - rotation * flow[0]) / divisor)

    def mixed(this, below, spread):
        shear = (this[0] - below[0]) ** 2 + (this[1] - below[1]) ** 2
        return 0.5 * spread + 0.5 * shear / (1.0 + shear)

    east, north = turned(flow_vector)
    after = turned(flow_after)
    ahead = turned(before[:2])
    below = tuple(jnp.concatenate([f[1:], g], axis=0) for f, g in zip((east, north), after))
    spreading = mixed((east, north), below, vertical_spreading)
    level_at = me * levels + jnp.arange(levels)
    kmix = jnp.where((level_at < depth - 1)[:, None, None], VERTICAL_MIX * spreading, 0.0)
    ahead_mix = VERTICAL_MIX * mixed(ahead, (east[:1], north[:1]), before[2])
    kmix = jnp.concatenate([jnp.where(me > 0, ahead_mix, 0.0), kmix], axis=0)
    thermal_carried = thermal_state + chemical_change(
        thermal_state,
        jnp.concatenate([thermal_state[:, 1:], thermal_east], axis=1),
        jnp.concatenate([thermal_west, thermal_state[:, :-1]], axis=1),
        east,
        north,
    )

    water = water_indicator.astype(jnp.float32)
    cap = -(-3 * across * lat // 4 // LANES) * LANES
    wet = (water_indicator > 0).astype(jnp.int32).reshape(-1, LANES)
    within = jnp.cumsum(wet, axis=1) - wet
    count = jnp.sum(wet, axis=1)
    offset = jnp.cumsum(count) - count
    tiles = offset // LANES
    shifts = offset % LANES
    slot = within + shifts[:, None]
    lane = jnp.arange(LANES, dtype=jnp.int32)
    hit = (slot % LANES)[:, None, :] == lane[None, :, None]
    gather = jnp.sum(
        jnp.where(hit & (wet > 0)[:, None, :], lane[None, None, :], 0), axis=2, dtype=jnp.int32
    )
    spread_at = slot % LANES
    spread_later = slot // LANES

    speeds = linear_exchange_speeds.reshape(n, held, n, held)
    precon = newton_preconditioner.reshape(n, held, n, held)
    speeds = relative(relative(speeds, me, n, 0), me, n, 2).reshape(tracers, tracers)
    precon = relative(relative(precon, me, n, 0), me, n, 2).reshape(tracers, tracers)
    rates = relative(absorption_speed.reshape(n, held), me, n, 0).reshape(tracers)
    row = jnp.arange(tracers * ROWS, dtype=jnp.int32)
    copy = (row[:, None] // ROWS == jnp.arange(tracers)[None, :]).astype(jnp.float32)
    same = row[:, None] % ROWS == row[None, :] % ROWS

    def widened(x):
        x = jnp.dot(copy, x, precision=lax.Precision.HIGHEST)
        x = jnp.dot(x, copy.T, precision=lax.Precision.HIGHEST)
        return halves_of(jnp.where(same, x, 0.0))

    speeds = widened(speeds)
    precon = widened(precon)
    rates = jnp.dot(
        copy, jnp.broadcast_to(rates[:, None], (tracers, lat)), precision=lax.Precision.HIGHEST
    )

    fields = (east, north, kmix, water, speeds, precon, rates, gather)
    edges = {}
    for q in range(parts):
        level, turn = {0: (0, 1), parts - 1: (nl - 1, n - 1)}.get(q, (None, 0))
        edges[q] = list(chunk_edges(blocks[q], level, turn))
        edges[q][0] = around(edges[q][0], "col", -1)
        edges[q][1] = around(edges[q][1], "col", 1)
    if parts == 1:
        edges[0].append(jnp.concatenate([b[:, -1:] for b in blocks[0][-1:] + blocks[0][:-1]], 0))
    above_all = shifted(edges[0][2], "sec", -1)
    below_all = shifted(edges[parts - 1][-1], "sec", 1)

    absorbs = {}
    returned = {}
    total = jnp.zeros((across, lat), jnp.float32)
    for q in order:
        below = (blocks[q - 1], nl - 1) if q > 0 else (below_all, 0)
        above = (blocks[q + 1], 0) if q < parts - 1 else (above_all, 0)
        *packed, absorbs[q], total = react_chunk(
            q, nl, me_at, tiles, shifts, blocks[q], below, above, edges[q][:2], fields, total,
            cap, q == order[-1],
        )
        returned[q] = []
        for d, x in enumerate(packed):
            returned[q].append(around(x, "sec", -d) if d else x)

    absorb = jnp.concatenate([absorbs[q] for q in range(parts)], axis=0)
    sun = shortwave[None, :]

    calls = [(q, tuple(range(n))) for q in order[:-1]]
    far = [0, *reach(n)]
    calls += [(order[-1], tuple(far[a:b])) for a, b in ((0, n // 2), (n // 2, n - 2), (n - 2, n))]
    solute_revised = None
    for k, (q, taken) in enumerate(calls):
        heat = (absorb, sun, thermal_carried) if k == len(calls) - 1 else None
        solute_revised, *thermal_revised = unpack_chunk(
            q, parts, me_at, tiles, returned[q], taken, solute_fields, water, spread_at,
            spread_later, solute_revised, cap, heat,
        )
    return thermal_revised[0], jnp.stack([east, north]), spreading, solute_revised


def solution(mesh):
    placed = (
        P("sec", "col", None),
        P(None, "sec", "col", None),
        P("sec", "col", None),
        P("sec", None, "col", None),
        P(),
        P(),
        P(),
        P("col", None),
    )
    return jax.shard_map(
        on_device,
        mesh=mesh,
        in_specs=placed,
        out_specs=(
            P("sec", "col", None),
            P(None, "sec", "col", None),
            P("sec", "col", None),
            P("sec", None, "col", None),
        ),
        check_vma=False,
    )
```

```python
import functools

import jax
import jax.numpy as jnp
from jax import lax
from jax.experimental import pallas as pl
from jax.experimental.pallas import tpu as pltpu
from jax.sharding import PartitionSpec as P


NEWTON = 2
CORIOLIS = 0.8
MIXING = 0.1
ADVECTION = 0.2
VERTICAL_MIX = 0.3
WATER_ABSORB = 0.02
PIGMENT_ABSORB = 0.06
CHLOROPHYLL_WARM = 10.0
LANES = 128
ROWS = 8
GAP = 8


def shifted(block, axis, distance):
    devices = range(lax.axis_size(axis))
    route = [(i - distance, i) for i in devices if i - distance in devices]
    return lax.ppermute(block, axis, route)


def around(block, axis, distance):
    count = lax.axis_size(axis)
    return lax.ppermute(block, axis, [(i, (i + distance) % count) for i in range(count)])


def chemical_change(center, eastern, western, east_flow, north_flow):
    northern = jnp.concatenate([center[..., 1:], center[..., -1:]], axis=-1)
    southern = jnp.concatenate([center[..., :1], center[..., :-1]], axis=-1)
    laplace = eastern + western + northern + southern - 4.0 * center
    return MIXING * laplace - 0.5 * ADVECTION * (
        east_flow * (eastern - western) + north_flow * (northern - southern)
    )


def edges_kernel(n, level, turn, *refs):
    cur = refs[:n]
    head, tail = refs[n : n + 2]
    held, nl, across, _ = cur[0].shape
    for d in range(n):
        for i in range(held):
            for l in range(nl):
                at = (d * held + i) * nl + l
                head[at : at + 1, :] = cur[d][i, l, 0:1, :]
                tail[at : at + 1, :] = cur[d][i, l, across - 1 : across, :]
    if level is not None:
        for d in range(n):
            refs[n + 2][d * held : (d + 1) * held] = cur[(d + turn) % n][:, level : level + 1]


def chunk_edges(blocks, level, turn):
    n = len(blocks)
    held, nl, across, lat = blocks[0].shape
    shapes = [jax.ShapeDtypeStruct((n * held * nl, lat), jnp.float32)] * 2
    if level is not None:
        shapes.append(jax.ShapeDtypeStruct((n * held, 1, across, lat), jnp.float32))
    return pl.pallas_call(
        functools.partial(edges_kernel, n, level, turn),
        in_specs=[pl.BlockSpec(memory_space=pltpu.VMEM)] * n,
        out_specs=[pl.BlockSpec(memory_space=pltpu.VMEM)] * len(shapes),
        out_shape=shapes,
        cost_estimate=pl.CostEstimate(
            flops=10**8, bytes_accessed=4 * n * blocks[0].size, transcendentals=0
        ),
        name="edges",
    )(*blocks)


def react_kernel(n, nl, q, closing, *refs):
    me_ref, tile_ref, shift_ref = refs[:3]
    cur = refs[3 : 3 + n]
    below = refs[3 + n : 3 + 2 * n]
    above = refs[3 + 2 * n : 3 + 3 * n]
    rest = refs[3 + 3 * n :]
    east_halo, west_halo, east, north, kmix, water, speeds, precon, rates, pick = rest[:10]
    before = rest[10]
    outs = rest[11 : 11 + n]
    absorbs, total = rest[11 + n : 13 + n]
    moved, done, packed = rest[13 + n :]
    held, _, across, lat = cur[0].shape
    tracers = n * held
    halves = across // ROWS
    pitch = across + GAP

    row_at = lax.broadcasted_iota(jnp.int32, (across, lat), 0)
    lane_at = lax.broadcasted_iota(jnp.int32, (across, lat), 1)
    wet = water[...]
    for l in range(nl):
        u = (0.5 * ADVECTION) * wet * east[l]
        v = (0.5 * ADVECTION) * wet * north[l]
        mix = MIXING * wet
        up = wet * kmix[q * nl + l + 1]
        down = wet * kmix[q * nl + l]
        to_east = mix - u
        to_west = mix + u
        last = lane_at == lat - 1
        first = lane_at == 0
        middle = 1.0 - 4.0 * mix - up - down
        to_north = mix - v
        to_south = mix + v
        middle = middle + jnp.where(last, to_north, 0.0) + jnp.where(first, to_south, 0.0)
        to_north = jnp.where(last, 0.0, to_north)
        to_south = jnp.where(first, 0.0, to_south)
        for d in range(n):
            for i in range(held):
                t = d * held + i
                c = cur[d][i, l]
                lower = cur[d][i, l - 1] if l > 0 else below[d][i, 0]
                upper = cur[d][i, l + 1] if l < nl - 1 else above[d][i, 0]
                at = t * nl + l
                e = jnp.where(
                    row_at == across - 1, east_halo[at : at + 1, :], pltpu.roll(c, across - 1, 0)
                )
                w = jnp.where(row_at == 0, west_halo[at : at + 1, :], pltpu.roll(c, 1, 0))
                value = middle * c + to_east * e + to_west * w
                value = value + to_north * pltpu.roll(c, lat - 1, 1) + to_south * pltpu.roll(c, 1, 1)
                value = value + up * upper + down * lower
                for h in range(halves):
                    moved[l * halves + h, t * ROWS : (t + 1) * ROWS, :] = value[
                        h * ROWS : (h + 1) * ROWS
                    ]

    def product(weights, x):
        high = x.astype(jnp.bfloat16)
        low = (x - high.astype(jnp.float32)).astype(jnp.bfloat16)
        return jnp.dot(
            weights[...],
            jnp.concatenate([high, low, high], axis=0),
            preferred_element_type=jnp.float32,
        )

    def uptake(x):
        square = x * x
        return rates[...] * (square / (1.0 + square))

    def react(j, carry):
        start = moved[j]
        current = start
        for step in range(NEWTON):
            misfit = uptake(current) - product(speeds, current)
            if step > 0:
                misfit = misfit + (current - start)
            current = current - product(precon, misfit)
        l = j // halves
        h = j % halves
        for t in range(tracers):
            at = pl.multiple_of((t * nl + l) * pitch + h * ROWS, ROWS)
            for s in range(lat // LANES):
                done[s, pl.ds(at, ROWS), :] = current[
                    t * ROWS : (t + 1) * ROWS, s * LANES : (s + 1) * LANES
                ]
        return carry

    lax.fori_loop(0, nl * halves, react, 0)

    me = me_ref[0]
    for s in range(lat // LANES):
        lanes = slice(s * LANES, (s + 1) * LANES)
        column = before[:, lanes]
        for l in range(nl):
            at = pl.multiple_of((me * (held * nl) + l) * pitch, ROWS)
            pigment = done[s, pl.ds(at, across), :]
            square = pigment * pigment
            absorb = WATER_ABSORB + PIGMENT_ABSORB * square / (1.0 + square)
            absorbs[l, :, lanes] = absorb
            column = column + absorb
        total[:, lanes] = column

    lane = lax.broadcasted_iota(jnp.int32, (ROWS, LANES), 1)
    parts = lat // LANES

    def pack(x, carry):
        for s in range(parts):
            segment = x * parts + s
            tile = pl.multiple_of(tile_ref[segment] * LANES, LANES)
            tail = pl.multiple_of(tile_ref[segment] * LANES + LANES, LANES)
            keep = lane < shift_ref[segment]
            index = jnp.broadcast_to(pick[pl.ds(segment, 1), :], (ROWS, LANES))
            for g in range(tracers * nl // ROWS):
                value = done[s, pl.ds(g * ROWS * pitch + x, ROWS, stride=pitch), :]
                value = jnp.take_along_axis(value, index, axis=1, mode="promise_in_bounds")
                here = (slice(g * ROWS, (g + 1) * ROWS), pl.ds(tile, LANES))
                packed[here] = jnp.where(keep, packed[here], value)
                packed[g * ROWS : (g + 1) * ROWS, pl.ds(tail, LANES)] = value
        return carry

    lax.fori_loop(0, across, pack, 0)
    cap = outs[0].shape[1] - (across * lat // (held * nl) if closing else 0)
    for d in range(n):
        outs[d][:, :cap] = packed[d * held * nl : (d + 1) * held * nl, :cap]
        if closing:
            for k in range(across // (held * nl)):
                outs[d][:, cap + k * lat : cap + (k + 1) * lat] = total[
                    k * held * nl : (k + 1) * held * nl, :
                ]


def react_chunk(q, nl, me, tiles, shifts, blocks, below, above, halos, fields, before, cap, closing):
    n = len(blocks)
    held, _, across, lat = blocks[0].shape
    east, north, kmix, water, speeds, precon, rates, pick = fields
    rows = n * held * ROWS
    whole = pl.BlockSpec(memory_space=pltpu.VMEM)

    def level(spec_at):
        return pl.BlockSpec((held, 1, across, lat), lambda i, *_: (0, spec_at, 0, 0))

    def all_of(x):
        return pl.BlockSpec(x.shape, lambda i, *_: (0,) * x.ndim)

    ins = list(blocks)
    specs = [all_of(b) for b in blocks]
    for source, at in (below, above):
        for d in range(n):
            if isinstance(source, list):
                ins.append(source[d])
                specs.append(level(at))
            else:
                ins.append(source)
                specs.append(
                    pl.BlockSpec((held, 1, across, lat), lambda i, *_, d=d: (d, 0, 0, 0))
                )
    for x in halos:
        ins.append(x)
        specs.append(all_of(x))
    for x in (east, north):
        ins.append(x)
        specs.append(pl.BlockSpec((nl, across, lat), lambda i, *_: (q, 0, 0)))
    for x in (kmix, water, speeds, precon, rates, pick, before):
        ins.append(x)
        specs.append(all_of(x))
    wide = cap + (across * lat // (held * nl) if closing else 0)
    shapes = [jax.ShapeDtypeStruct((held * nl, wide), jnp.float32)] * n
    shapes.append(jax.ShapeDtypeStruct((nl, across, lat), jnp.float32))
    shapes.append(jax.ShapeDtypeStruct((across, lat), jnp.float32))
    lanes = (cap // LANES + 2) * LANES
    flops = 2 * 12 * rows * rows * lat * nl * (across // ROWS)
    return pl.pallas_call(
        functools.partial(react_kernel, n, nl, q, closing),
        grid_spec=pltpu.PrefetchScalarGridSpec(
            num_scalar_prefetch=3,
            grid=(1,),
            in_specs=specs,
            out_specs=[
                pl.BlockSpec(s.shape, lambda i, *_, k=len(s.shape): (0,) * k) for s in shapes
            ],
            scratch_shapes=[
                pltpu.VMEM((nl * (across // ROWS), rows, lat), jnp.float32),
                pltpu.VMEM((lat // LANES, n * held * nl * (across + GAP), LANES), jnp.float32),
                pltpu.VMEM((n * held * nl, lanes), jnp.float32),
            ],
        ),
        out_shape=shapes,
        cost_estimate=pl.CostEstimate(
            flops=flops, bytes_accessed=4 * 3 * rows * nl * across * lat // ROWS, transcendentals=0
        ),
        name="react",
    )(me, tiles, shifts, *ins)


def unpack_kernel(n, nl, cap, at_level, has_base, closing, *refs):
    me_ref, tile_ref = refs[:2]
    received = refs[2 : 2 + n]
    solute, *small = refs[2 + n : 6 + n + 3 * closing]
    rest = refs[6 + n + 3 * closing + has_base :]
    out, *rest = rest
    if closing:
        warmed_out, *rest = rest
    slots, cells, spread, sems, *rest = rest
    held, depth, across, lat = solute.shape
    levels = depth // n
    pitch = across + GAP
    here = me_ref[0]
    lanes_in = received[0].shape[1]
    copies = [
        pltpu.make_async_copy(source, target, sems.at[0, n + k])
        for k, (source, target) in enumerate(zip(small, rest))
    ]

    def place(d):
        return pl.ds(lax.rem(here + d, n) * levels + at_level, nl)

    def packed_in(d, source):
        return pltpu.make_async_copy(
            source, slots.at[d, :, pl.ds(0, lanes_in)], sems.at[0, d]
        )

    def block_in(d):
        return pltpu.make_async_copy(solute.at[:, place(d)], cells.at[d], sems.at[1, d])

    def block_out(d):
        return pltpu.make_async_copy(cells.at[d], out.at[:, place(d)], sems.at[2, d])

    for copy in copies[:3]:
        copy.start()
    for d in range(n):
        packed_in(d, received[d]).start()
        block_in(d).start()
    for copy in copies[3:]:
        copy.start()
    for copy in copies[:3]:
        copy.wait()
    water, pick, second = rest[:3]
    wet = water[...] > 0.5

    def unpack(d, carry):
        packed_in(d, received[0]).wait()
        block_in(d).wait()
        spread_block(d, tile_ref, pick, second, slots, spread, held * nl, across, lat)
        for i in range(held):
            for l in range(nl):
                at = (i * nl + l) * pitch
                for s in range(lat // LANES):
                    lanes = slice(s * LANES, (s + 1) * LANES)
                    cells[d, i, l, :, lanes] = jnp.where(
                        wet[:, lanes], spread[s, at : at + across, :], cells[d, i, l, :, lanes]
                    )
        block_out(d).start()
        return carry

    lax.fori_loop(0, n, unpack, 0)
    if closing:
        for copy in copies[3:]:
            copy.wait()
        absorb, sun, carried, warmed = rest[3:]
        size = held * nl
        for k in range(across // size):
            lane = slice(cap + k * lat, cap + (k + 1) * lat)
            row = slice(k * size, (k + 1) * size)
            over = jnp.zeros((size, lat), jnp.float32)
            for d in range(1, n):
                above = lax.rem(here + d, n) < here
                over = over + jnp.where(above, slots[d, :, lane], 0.0)
            light = sun[...] * (CHLOROPHYLL_WARM * water[row, :])
            coming = jnp.exp(-over)
            for l in range(absorb.shape[0]):
                over = over + absorb[l, row, :]
                left = jnp.exp(-over)
                warmed[l, row, :] = carried[l, row, :] + light * (coming - left)
                coming = left
        warm = pltpu.make_async_copy(warmed, warmed_out, sems.at[1, n])
        warm.start()
        warm.wait()
    for d in range(n):
        block_out(d).wait()


def spread_block(k, tile_ref, pick, second, slots, spread, rows, across, lat):
    pitch = across + GAP
    parts = lat // LANES
    for x in range(across):
        for s in range(parts):
            segment = x * parts + s
            tile = pl.multiple_of(tile_ref[segment] * LANES, LANES)
            tail = pl.multiple_of(tile_ref[segment] * LANES + LANES, LANES)
            index = jnp.broadcast_to(pick[segment : segment + 1, :], (ROWS, LANES))
            later = jnp.broadcast_to(second[segment : segment + 1, :], (ROWS, LANES)) > 0
            for g in range(rows // ROWS):
                group = slice(g * ROWS, (g + 1) * ROWS)
                a = jnp.take_along_axis(
                    slots[k, group, pl.ds(tile, LANES)], index, axis=1, mode="promise_in_bounds"
                )
                b = jnp.take_along_axis(
                    slots[k, group, pl.ds(tail, LANES)], index, axis=1, mode="promise_in_bounds"
                )
                spread[s, pl.ds(g * ROWS * pitch + x, ROWS, stride=pitch), :] = jnp.where(
                    later, b, a
                )


def unpack_chunk(q, parts, me, tiles, returned, solute, small, base, cap, heat=()):
    n = len(returned)
    held, depth, across, lat = solute.shape
    nl = depth // n // parts
    ins = [*returned, solute, *small, *heat]
    shapes = [jax.ShapeDtypeStruct(solute.shape, jnp.float32)]
    scratch = [pltpu.VMEM(x.shape, x.dtype) for x in (*small, *heat)]
    if heat:
        shapes.append(jax.ShapeDtypeStruct(heat[-1].shape, jnp.float32))
        scratch.append(scratch[-1])
    aliases = {}
    if base is not None:
        aliases = {2 + len(ins): 0}
        ins.append(base)
    apart = pl.BlockSpec(memory_space=pltpu.HBM)
    slot_lanes = max(cap + 2 * LANES, returned[0].shape[1])
    return pl.pallas_call(
        functools.partial(
            unpack_kernel, n, nl, cap, q * nl, base is not None, len(heat) > 0
        ),
        grid_spec=pltpu.PrefetchScalarGridSpec(
            num_scalar_prefetch=2,
            grid=(1,),
            in_specs=[apart] * len(ins),
            out_specs=[apart] * len(shapes),
            scratch_shapes=[
                pltpu.VMEM((n, held * nl, slot_lanes), jnp.float32),
                pltpu.VMEM((n, held, nl, across, lat), jnp.float32),
                pltpu.VMEM((lat // LANES, held * nl * (across + GAP), LANES), jnp.float32),
                pltpu.SemaphoreType.DMA((3, n + len(small) + len(heat))),
                *scratch,
            ],
        ),
        out_shape=shapes,
        input_output_aliases=aliases,
        cost_estimate=pl.CostEstimate(
            flops=100 * solute.size, bytes_accessed=12 * solute.size // parts, transcendentals=0
        ),
        name="unpack",
    )(me, tiles, *ins)


def relative(x, me, n, axis):
    x = jnp.flip(x, axis)
    return lax.dynamic_slice_in_dim(jnp.concatenate([x, x], axis), n - 1 - me, n, axis)


def halves_of(x):
    high = lax.reduce_precision(x, 8, 7)
    low = x - high
    return jnp.concatenate([high, high, low], axis=1).astype(jnp.bfloat16)


def plan(held, levels):
    nl = max(levels // 4, ROWS // held)
    parts = levels // nl
    inner = list(range(1, parts - 1))
    return nl, parts, inner + [q for q in (parts - 1, 0) if q not in inner][: parts - len(inner)]


def reach(n):
    return sorted(range(1, n), key=lambda d: (-min(d, n - d), d))


def on_device(
    thermal_state,
    flow_vector,
    vertical_spreading,
    solute_fields,
    linear_exchange_speeds,
    newton_preconditioner,
    absorption_speed,
    water_indicator,
):
    n = lax.axis_size("sec")
    me = lax.axis_index("sec")
    held, depth, across, lat = solute_fields.shape
    tracers = n * held
    levels = depth // n
    nl, parts, order = plan(held, levels)
    me_at = jnp.reshape(me, (1,)).astype(jnp.int32)

    blocks = {}
    raw = solute_fields
    for q in range(parts):
        sends = {}
        for d in reach(n):
            to = lax.rem(me + d, n)
            sends[d] = lax.dynamic_slice_in_dim(raw, to * levels + q * nl, nl, 1)
        if q == 0:
            raw, sends = lax.optimization_barrier((raw, sends))
        blocks[q] = [lax.dynamic_slice_in_dim(raw, me * levels + q * nl, nl, 1)]
        for d in range(1, n):
            blocks[q].append(around(sends[d], "sec", d))

    flow_after = shifted(flow_vector[:, :1], "sec", -1)
    before = shifted(
        jnp.concatenate([flow_vector[:, -1:], vertical_spreading[None, -1:]], axis=0), "sec", 1
    )
    thermal_west = around(thermal_state[:, -1:], "col", 1)
    thermal_east = around(thermal_state[:, :1], "col", -1)

    latitude = jnp.pi * (jnp.arange(lat).astype(jnp.float32) + 0.5) / lat - jnp.pi / 2
    rotation = CORIOLIS * jnp.sin(latitude)
    shortwave = jnp.cos(latitude)
    divisor = 1.0 + rotation * rotation

    def turned(flow):
        return ((flow[0] + rotation * flow[1]) / divisor, (flow[1] - rotation * flow[0]) / divisor)

    def mixed(this, below, spread):
        shear = (this[0] - below[0]) ** 2 + (this[1] - below[1]) ** 2
        return 0.5 * spread + 0.5 * shear / (1.0 + shear)

    east, north = turned(flow_vector)
    after = turned(flow_after)
    ahead = turned(before[:2])
    below = tuple(jnp.concatenate([f[1:], g], axis=0) for f, g in zip((east, north), after))
    spreading = mixed((east, north), below, vertical_spreading)
    level_at = me * levels + jnp.arange(levels)
    kmix = jnp.where((level_at < depth - 1)[:, None, None], VERTICAL_MIX * spreading, 0.0)
    ahead_mix = VERTICAL_MIX * mixed(ahead, (east[:1], north[:1]), before[2])
    kmix = jnp.concatenate([jnp.where(me > 0, ahead_mix, 0.0), kmix], axis=0)
    thermal_carried = thermal_state + chemical_change(
        thermal_state,
        jnp.concatenate([thermal_state[:, 1:], thermal_east], axis=1),
        jnp.concatenate([thermal_west, thermal_state[:, :-1]], axis=1),
        east,
        north,
    )

    water = water_indicator.astype(jnp.float32)
    cap = -(-3 * across * lat // 4 // LANES) * LANES
    wet = (water_indicator > 0).astype(jnp.int32).reshape(-1, LANES)
    within = jnp.cumsum(wet, axis=1) - wet
    count = jnp.sum(wet, axis=1)
    offset = jnp.cumsum(count) - count
    tiles = offset // LANES
    shifts = offset % LANES
    slot = within + shifts[:, None]
    lane = jnp.arange(LANES, dtype=jnp.int32)
    hit = (slot % LANES)[:, None, :] == lane[None, :, None]
    gather = jnp.sum(
        jnp.where(hit & (wet > 0)[:, None, :], lane[None, None, :], 0), axis=2, dtype=jnp.int32
    )
    spread_at = slot % LANES
    spread_later = slot // LANES

    speeds = linear_exchange_speeds.reshape(n, held, n, held)
    precon = newton_preconditioner.reshape(n, held, n, held)
    speeds = relative(relative(speeds, me, n, 0), me, n, 2).reshape(tracers, tracers)
    precon = relative(relative(precon, me, n, 0), me, n, 2).reshape(tracers, tracers)
    rates = relative(absorption_speed.reshape(n, held), me, n, 0).reshape(tracers)
    row = jnp.arange(tracers * ROWS, dtype=jnp.int32)
    copy = (row[:, None] // ROWS == jnp.arange(tracers)[None, :]).astype(jnp.float32)
    same = row[:, None] % ROWS == row[None, :] % ROWS

    def widened(x):
        x = jnp.dot(copy, x, precision=lax.Precision.HIGHEST)
        x = jnp.dot(x, copy.T, precision=lax.Precision.HIGHEST)
        return halves_of(jnp.where(same, x, 0.0))

    speeds = widened(speeds)
    precon = widened(precon)
    rates = jnp.dot(
        copy, jnp.broadcast_to(rates[:, None], (tracers, lat)), precision=lax.Precision.HIGHEST
    )

    fields = (east, north, kmix, water, speeds, precon, rates, gather)
    edges = {}
    for q in range(parts):
        level, turn = {0: (0, 1), parts - 1: (nl - 1, n - 1)}.get(q, (None, 0))
        edges[q] = list(chunk_edges(blocks[q], level, turn))
        edges[q][0] = around(edges[q][0], "col", -1)
        edges[q][1] = around(edges[q][1], "col", 1)
    if parts == 1:
        edges[0].append(jnp.concatenate([b[:, -1:] for b in blocks[0][-1:] + blocks[0][:-1]], 0))
    above_all = shifted(edges[0][2], "sec", -1)
    below_all = shifted(edges[parts - 1][-1], "sec", 1)

    absorbs = {}
    returned = {}
    total = jnp.zeros((across, lat), jnp.float32)
    for q in order:
        below = (blocks[q - 1], nl - 1) if q > 0 else (below_all, 0)
        above = (blocks[q + 1], 0) if q < parts - 1 else (above_all, 0)
        *packed, absorbs[q], total = react_chunk(
            q, nl, me_at, tiles, shifts, blocks[q], below, above, edges[q][:2], fields, total,
            cap, q == order[-1],
        )
        returned[q] = []
        for d, x in enumerate(packed):
            returned[q].append(around(x, "sec", -d) if d else x)

    absorb = jnp.concatenate([absorbs[q] for q in range(parts)], axis=0)
    sun = shortwave[None, :]

    small = (water, spread_at, spread_later)
    solute_revised = None
    for q in order:
        heat = (absorb, sun, thermal_carried) if q == order[-1] else ()
        solute_revised, *thermal_revised = unpack_chunk(
            q, parts, me_at, tiles, returned[q], solute_fields, small, solute_revised, cap, heat
        )
    return thermal_revised[0], jnp.stack([east, north]), spreading, solute_revised


def solution(mesh):
    placed = (
        P("sec", "col", None),
        P(None, "sec", "col", None),
        P("sec", "col", None),
        P("sec", None, "col", None),
        P(),
        P(),
        P(),
        P("col", None),
    )
    return jax.shard_map(
        on_device,
        mesh=mesh,
        in_specs=placed,
        out_specs=(
            P("sec", "col", None),
            P(None, "sec", "col", None),
            P("sec", "col", None),
            P("sec", None, "col", None),
        ),
        check_vma=False,
    )
```

```python
import functools

import jax
import jax.numpy as jnp
from jax import lax
from jax.experimental import pallas as pl
from jax.experimental.pallas import tpu as pltpu
from jax.sharding import PartitionSpec as P


NEWTON = 2
CORIOLIS = 0.8
MIXING = 0.1
ADVECTION = 0.2
VERTICAL_MIX = 0.3
WATER_ABSORB = 0.02
PIGMENT_ABSORB = 0.06
CHLOROPHYLL_WARM = 10.0
LANES = 128
ROWS = 8
GAP = 8


def shifted(block, axis, distance):
    devices = range(lax.axis_size(axis))
    route = [(i - distance, i) for i in devices if i - distance in devices]
    return lax.ppermute(block, axis, route)


def around(block, axis, distance):
    count = lax.axis_size(axis)
    return lax.ppermute(block, axis, [(i, (i + distance) % count) for i in range(count)])


def chemical_change(center, eastern, western, east_flow, north_flow):
    northern = jnp.concatenate([center[..., 1:], center[..., -1:]], axis=-1)
    southern = jnp.concatenate([center[..., :1], center[..., :-1]], axis=-1)
    laplace = eastern + western + northern + southern - 4.0 * center
    return MIXING * laplace - 0.5 * ADVECTION * (
        east_flow * (eastern - western) + north_flow * (northern - southern)
    )


def edges_kernel(n, level, turn, *refs):
    cur = refs[:n]
    head, tail = refs[n : n + 2]
    held, nl, across, _ = cur[0].shape
    for d in range(n):
        for i in range(held):
            for l in range(nl):
                at = (d * held + i) * nl + l
                head[at : at + 1, :] = cur[d][i, l, 0:1, :]
                tail[at : at + 1, :] = cur[d][i, l, across - 1 : across, :]
    if level is not None:
        for d in range(n):
            refs[n + 2][d * held : (d + 1) * held] = cur[(d + turn) % n][:, level : level + 1]


def chunk_edges(blocks, level, turn):
    n = len(blocks)
    held, nl, across, lat = blocks[0].shape
    shapes = [jax.ShapeDtypeStruct((n * held * nl, lat), jnp.float32)] * 2
    if level is not None:
        shapes.append(jax.ShapeDtypeStruct((n * held, 1, across, lat), jnp.float32))
    return pl.pallas_call(
        functools.partial(edges_kernel, n, level, turn),
        in_specs=[pl.BlockSpec(memory_space=pltpu.VMEM)] * n,
        out_specs=[pl.BlockSpec(memory_space=pltpu.VMEM)] * len(shapes),
        out_shape=shapes,
        cost_estimate=pl.CostEstimate(
            flops=10**8, bytes_accessed=4 * n * blocks[0].size, transcendentals=0
        ),
        name="edges",
    )(*blocks)


def react_kernel(n, nl, q, closing, *refs):
    me_ref, tile_ref, shift_ref = refs[:3]
    cur = refs[3 : 3 + n]
    below = refs[3 + n : 3 + 2 * n]
    above = refs[3 + 2 * n : 3 + 3 * n]
    rest = refs[3 + 3 * n :]
    east_halo, west_halo, east, north, kmix, water, speeds, precon, rates, pick = rest[:10]
    before = rest[10]
    outs = rest[11 : 11 + n]
    absorbs, total = rest[11 + n : 13 + n]
    moved, done, packed = rest[13 + n :]
    held, _, across, lat = cur[0].shape
    tracers = n * held
    halves = across // ROWS
    pitch = across + GAP

    row_at = lax.broadcasted_iota(jnp.int32, (across, lat), 0)
    lane_at = lax.broadcasted_iota(jnp.int32, (across, lat), 1)
    wet = water[...]
    for l in range(nl):
        u = (0.5 * ADVECTION) * wet * east[l]
        v = (0.5 * ADVECTION) * wet * north[l]
        mix = MIXING * wet
        up = wet * kmix[q * nl + l + 1]
        down = wet * kmix[q * nl + l]
        to_east = mix - u
        to_west = mix + u
        last = lane_at == lat - 1
        first = lane_at == 0
        middle = 1.0 - 4.0 * mix - up - down
        to_north = mix - v
        to_south = mix + v
        middle = middle + jnp.where(last, to_north, 0.0) + jnp.where(first, to_south, 0.0)
        to_north = jnp.where(last, 0.0, to_north)
        to_south = jnp.where(first, 0.0, to_south)
        for d in range(n):
            for i in range(held):
                t = d * held + i
                c = cur[d][i, l]
                lower = cur[d][i, l - 1] if l > 0 else below[d][i, 0]
                upper = cur[d][i, l + 1] if l < nl - 1 else above[d][i, 0]
                at = t * nl + l
                e = jnp.where(
                    row_at == across - 1, east_halo[at : at + 1, :], pltpu.roll(c, across - 1, 0)
                )
                w = jnp.where(row_at == 0, west_halo[at : at + 1, :], pltpu.roll(c, 1, 0))
                value = middle * c + to_east * e + to_west * w
                value = value + to_north * pltpu.roll(c, lat - 1, 1) + to_south * pltpu.roll(c, 1, 1)
                value = value + up * upper + down * lower
                for h in range(halves):
                    moved[l * halves + h, t * ROWS : (t + 1) * ROWS, :] = value[
                        h * ROWS : (h + 1) * ROWS
                    ]

    def product(weights, x):
        high = x.astype(jnp.bfloat16)
        low = (x - high.astype(jnp.float32)).astype(jnp.bfloat16)
        return jnp.dot(
            weights[...],
            jnp.concatenate([high, low, high], axis=0),
            preferred_element_type=jnp.float32,
        )

    def uptake(x):
        square = x * x
        return rates[...] * (square / (1.0 + square))

    def react(j, carry):
        start = moved[j]
        current = start
        for step in range(NEWTON):
            misfit = uptake(current) - product(speeds, current)
            if step > 0:
                misfit = misfit + (current - start)
            current = current - product(precon, misfit)
        l = j // halves
        h = j % halves
        for t in range(tracers):
            at = pl.multiple_of((t * nl + l) * pitch + h * ROWS, ROWS)
            for s in range(lat // LANES):
                done[s, pl.ds(at, ROWS), :] = current[
                    t * ROWS : (t + 1) * ROWS, s * LANES : (s + 1) * LANES
                ]
        return carry

    lax.fori_loop(0, nl * halves, react, 0)

    me = me_ref[0]
    for s in range(lat // LANES):
        lanes = slice(s * LANES, (s + 1) * LANES)
        column = before[:, lanes]
        for l in range(nl):
            at = pl.multiple_of((me * (held * nl) + l) * pitch, ROWS)
            pigment = done[s, pl.ds(at, across), :]
            square = pigment * pigment
            absorb = WATER_ABSORB + PIGMENT_ABSORB * square / (1.0 + square)
            absorbs[l, :, lanes] = absorb
            column = column + absorb
        total[:, lanes] = column

    lane = lax.broadcasted_iota(jnp.int32, (ROWS, LANES), 1)
    parts = lat // LANES

    def pack(x, carry):
        for s in range(parts):
            segment = x * parts + s
            tile = pl.multiple_of(tile_ref[segment] * LANES, LANES)
            tail = pl.multiple_of(tile_ref[segment] * LANES + LANES, LANES)
            keep = lane < shift_ref[segment]
            index = jnp.broadcast_to(pick[pl.ds(segment, 1), :], (ROWS, LANES))
            for g in range(tracers * nl // ROWS):
                value = done[s, pl.ds(g * ROWS * pitch + x, ROWS, stride=pitch), :]
                value = jnp.take_along_axis(value, index, axis=1, mode="promise_in_bounds")
                here = (slice(g * ROWS, (g + 1) * ROWS), pl.ds(tile, LANES))
                packed[here] = jnp.where(keep, packed[here], value)
                packed[g * ROWS : (g + 1) * ROWS, pl.ds(tail, LANES)] = value
        return carry

    lax.fori_loop(0, across, pack, 0)
    cap = outs[0].shape[1] - (across * lat // (held * nl) if closing else 0)
    for d in range(n):
        outs[d][:, :cap] = packed[d * held * nl : (d + 1) * held * nl, :cap]
        if closing:
            for k in range(across // (held * nl)):
                outs[d][:, cap + k * lat : cap + (k + 1) * lat] = total[
                    k * held * nl : (k + 1) * held * nl, :
                ]


def react_chunk(q, nl, me, tiles, shifts, blocks, below, above, halos, fields, before, cap, closing):
    n = len(blocks)
    held, _, across, lat = blocks[0].shape
    east, north, kmix, water, speeds, precon, rates, pick = fields
    rows = n * held * ROWS
    whole = pl.BlockSpec(memory_space=pltpu.VMEM)

    def level(spec_at):
        return pl.BlockSpec((held, 1, across, lat), lambda i, *_: (0, spec_at, 0, 0))

    def all_of(x):
        return pl.BlockSpec(x.shape, lambda i, *_: (0,) * x.ndim)

    ins = list(blocks)
    specs = [all_of(b) for b in blocks]
    for source, at in (below, above):
        for d in range(n):
            if isinstance(source, list):
                ins.append(source[d])
                specs.append(level(at))
            else:
                ins.append(source)
                specs.append(
                    pl.BlockSpec((held, 1, across, lat), lambda i, *_, d=d: (d, 0, 0, 0))
                )
    for x in halos:
        ins.append(x)
        specs.append(all_of(x))
    for x in (east, north):
        ins.append(x)
        specs.append(pl.BlockSpec((nl, across, lat), lambda i, *_: (q, 0, 0)))
    for x in (kmix, water, speeds, precon, rates, pick, before):
        ins.append(x)
        specs.append(all_of(x))
    wide = cap + (across * lat // (held * nl) if closing else 0)
    shapes = [jax.ShapeDtypeStruct((held * nl, wide), jnp.float32)] * n
    shapes.append(jax.ShapeDtypeStruct((nl, across, lat), jnp.float32))
    shapes.append(jax.ShapeDtypeStruct((across, lat), jnp.float32))
    lanes = (cap // LANES + 2) * LANES
    flops = 2 * 12 * rows * rows * lat * nl * (across // ROWS)
    return pl.pallas_call(
        functools.partial(react_kernel, n, nl, q, closing),
        grid_spec=pltpu.PrefetchScalarGridSpec(
            num_scalar_prefetch=3,
            grid=(1,),
            in_specs=specs,
            out_specs=[
                pl.BlockSpec(s.shape, lambda i, *_, k=len(s.shape): (0,) * k) for s in shapes
            ],
            scratch_shapes=[
                pltpu.VMEM((nl * (across // ROWS), rows, lat), jnp.float32),
                pltpu.VMEM((lat // LANES, n * held * nl * (across + GAP), LANES), jnp.float32),
                pltpu.VMEM((n * held * nl, lanes), jnp.float32),
            ],
        ),
        out_shape=shapes,
        cost_estimate=pl.CostEstimate(
            flops=flops, bytes_accessed=4 * 3 * rows * nl * across * lat // ROWS, transcendentals=0
        ),
        name="react",
    )(me, tiles, shifts, *ins)


def unpack_kernel(n, nl, cap, at_level, has_base, closing, *refs):
    me_ref, tile_ref = refs[:2]
    received = refs[2 : 2 + n]
    solute, *small = refs[2 + n : 6 + n + 3 * closing]
    rest = refs[6 + n + 3 * closing + has_base :]
    out, *rest = rest
    if closing:
        warmed_out, *rest = rest
    slots, cells, spread, sems, *rest = rest
    held, depth, across, lat = solute.shape
    levels = depth // n
    pitch = across + GAP
    here = me_ref[0]
    lanes_in = received[0].shape[1]
    copies = [
        pltpu.make_async_copy(source, target, sems.at[0, n + k])
        for k, (source, target) in enumerate(zip(small, rest))
    ]

    def place(d):
        return pl.ds(lax.rem(here + d, n) * levels + at_level, nl)

    def packed_in(d, source):
        return pltpu.make_async_copy(
            source, slots.at[d, :, pl.ds(0, lanes_in)], sems.at[0, d]
        )

    def block_in(d):
        return pltpu.make_async_copy(solute.at[:, place(d)], cells.at[d], sems.at[1, d])

    def block_out(d):
        return pltpu.make_async_copy(cells.at[d], out.at[:, place(d)], sems.at[2, d])

    for copy in copies[:3]:
        copy.start()
    for d in range(n):
        packed_in(d, received[d]).start()
        block_in(d).start()
    for copy in copies[3:]:
        copy.start()
    for copy in copies[:3]:
        copy.wait()
    water, pick, second = rest[:3]
    wet = water[...] > 0.5

    def unpack(d, carry, arrived=False):
        if not arrived:
            packed_in(d, received[0]).wait()
        block_in(d).wait()
        spread_block(d, tile_ref, pick, second, slots, spread, held * nl, across, lat)
        for i in range(held):
            for l in range(nl):
                at = (i * nl + l) * pitch
                for s in range(lat // LANES):
                    lanes = slice(s * LANES, (s + 1) * LANES)
                    cells[d, i, l, :, lanes] = jnp.where(
                        wet[:, lanes], spread[s, at : at + across, :], cells[d, i, l, :, lanes]
                    )
        block_out(d).start()
        return carry

    early = n - 3 if closing else n
    lax.fori_loop(0, early, unpack, 0)
    if closing:
        for d in range(early, n):
            packed_in(d, received[0]).wait()
        for copy in copies[3:]:
            copy.wait()
        absorb, sun, carried, warmed = rest[3:]
        size = held * nl
        for k in range(across // size):
            lane = slice(cap + k * lat, cap + (k + 1) * lat)
            row = slice(k * size, (k + 1) * size)
            over = jnp.zeros((size, lat), jnp.float32)
            for d in range(1, n):
                above = lax.rem(here + d, n) < here
                over = over + jnp.where(above, slots[d, :, lane], 0.0)
            light = sun[...] * (CHLOROPHYLL_WARM * water[row, :])
            coming = jnp.exp(-over)
            for l in range(absorb.shape[0]):
                over = over + absorb[l, row, :]
                left = jnp.exp(-over)
                warmed[l, row, :] = carried[l, row, :] + light * (coming - left)
                coming = left
        warm = pltpu.make_async_copy(warmed, warmed_out, sems.at[1, n])
        warm.start()
        lax.fori_loop(early, n, functools.partial(unpack, arrived=True), 0)
        warm.wait()
    for d in range(n):
        block_out(d).wait()


def spread_block(k, tile_ref, pick, second, slots, spread, rows, across, lat):
    pitch = across + GAP
    parts = lat // LANES
    for x in range(across):
        for s in range(parts):
            segment = x * parts + s
            tile = pl.multiple_of(tile_ref[segment] * LANES, LANES)
            tail = pl.multiple_of(tile_ref[segment] * LANES + LANES, LANES)
            index = jnp.broadcast_to(pick[segment : segment + 1, :], (ROWS, LANES))
            later = jnp.broadcast_to(second[segment : segment + 1, :], (ROWS, LANES)) > 0
            for g in range(rows // ROWS):
                group = slice(g * ROWS, (g + 1) * ROWS)
                a = jnp.take_along_axis(
                    slots[k, group, pl.ds(tile, LANES)], index, axis=1, mode="promise_in_bounds"
                )
                b = jnp.take_along_axis(
                    slots[k, group, pl.ds(tail, LANES)], index, axis=1, mode="promise_in_bounds"
                )
                spread[s, pl.ds(g * ROWS * pitch + x, ROWS, stride=pitch), :] = jnp.where(
                    later, b, a
                )


def unpack_chunk(q, parts, me, tiles, returned, solute, small, base, cap, heat=()):
    n = len(returned)
    held, depth, across, lat = solute.shape
    nl = depth // n // parts
    ins = [*returned, solute, *small, *heat]
    shapes = [jax.ShapeDtypeStruct(solute.shape, jnp.float32)]
    scratch = [pltpu.VMEM(x.shape, x.dtype) for x in (*small, *heat)]
    if heat:
        shapes.append(jax.ShapeDtypeStruct(heat[-1].shape, jnp.float32))
        scratch.append(scratch[-1])
    aliases = {}
    if base is not None:
        aliases = {2 + len(ins): 0}
        ins.append(base)
    apart = pl.BlockSpec(memory_space=pltpu.HBM)
    slot_lanes = max(cap + 2 * LANES, returned[0].shape[1])
    return pl.pallas_call(
        functools.partial(
            unpack_kernel, n, nl, cap, q * nl, base is not None, len(heat) > 0
        ),
        grid_spec=pltpu.PrefetchScalarGridSpec(
            num_scalar_prefetch=2,
            grid=(1,),
            in_specs=[apart] * len(ins),
            out_specs=[apart] * len(shapes),
            scratch_shapes=[
                pltpu.VMEM((n, held * nl, slot_lanes), jnp.float32),
                pltpu.VMEM((n, held, nl, across, lat), jnp.float32),
                pltpu.VMEM((lat // LANES, held * nl * (across + GAP), LANES), jnp.float32),
                pltpu.SemaphoreType.DMA((3, n + len(small) + len(heat))),
                *scratch,
            ],
        ),
        out_shape=shapes,
        input_output_aliases=aliases,
        cost_estimate=pl.CostEstimate(
            flops=100 * solute.size, bytes_accessed=12 * solute.size // parts, transcendentals=0
        ),
        name="unpack",
    )(me, tiles, *ins)


def relative(x, me, n, axis):
    x = jnp.flip(x, axis)
    return lax.dynamic_slice_in_dim(jnp.concatenate([x, x], axis), n - 1 - me, n, axis)


def halves_of(x):
    high = lax.reduce_precision(x, 8, 7)
    low = x - high
    return jnp.concatenate([high, high, low], axis=1).astype(jnp.bfloat16)


def plan(held, levels):
    nl = max(levels // 4, ROWS // held)
    parts = levels // nl
    inner = list(range(1, parts - 1))
    return nl, parts, inner + [q for q in (parts - 1, 0) if q not in inner][: parts - len(inner)]


def reach(n):
    return sorted(range(1, n), key=lambda d: (-min(d, n - d), d))


def on_device(
    thermal_state,
    flow_vector,
    vertical_spreading,
    solute_fields,
    linear_exchange_speeds,
    newton_preconditioner,
    absorption_speed,
    water_indicator,
):
    n = lax.axis_size("sec")
    me = lax.axis_index("sec")
    held, depth, across, lat = solute_fields.shape
    tracers = n * held
    levels = depth // n
    nl, parts, order = plan(held, levels)
    me_at = jnp.reshape(me, (1,)).astype(jnp.int32)

    blocks = {}
    raw = solute_fields
    for q in range(parts):
        sends = {}
        for d in reach(n):
            to = lax.rem(me + d, n)
            sends[d] = lax.dynamic_slice_in_dim(raw, to * levels + q * nl, nl, 1)
        if q == 0:
            raw, sends = lax.optimization_barrier((raw, sends))
        blocks[q] = [lax.dynamic_slice_in_dim(raw, me * levels + q * nl, nl, 1)]
        for d in range(1, n):
            blocks[q].append(around(sends[d], "sec", d))

    flow_after = shifted(flow_vector[:, :1], "sec", -1)
    before = shifted(
        jnp.concatenate([flow_vector[:, -1:], vertical_spreading[None, -1:]], axis=0), "sec", 1
    )
    thermal_west = around(thermal_state[:, -1:], "col", 1)
    thermal_east = around(thermal_state[:, :1], "col", -1)

    latitude = jnp.pi * (jnp.arange(lat).astype(jnp.float32) + 0.5) / lat - jnp.pi / 2
    rotation = CORIOLIS * jnp.sin(latitude)
    shortwave = jnp.cos(latitude)
    divisor = 1.0 + rotation * rotation

    def turned(flow):
        return ((flow[0] + rotation * flow[1]) / divisor, (flow[1] - rotation * flow[0]) / divisor)

    def mixed(this, below, spread):
        shear = (this[0] - below[0]) ** 2 + (this[1] - below[1]) ** 2
        return 0.5 * spread + 0.5 * shear / (1.0 + shear)

    east, north = turned(flow_vector)
    after = turned(flow_after)
    ahead = turned(before[:2])
    below = tuple(jnp.concatenate([f[1:], g], axis=0) for f, g in zip((east, north), after))
    spreading = mixed((east, north), below, vertical_spreading)
    level_at = me * levels + jnp.arange(levels)
    kmix = jnp.where((level_at < depth - 1)[:, None, None], VERTICAL_MIX * spreading, 0.0)
    ahead_mix = VERTICAL_MIX * mixed(ahead, (east[:1], north[:1]), before[2])
    kmix = jnp.concatenate([jnp.where(me > 0, ahead_mix, 0.0), kmix], axis=0)
    thermal_carried = thermal_state + chemical_change(
        thermal_state,
        jnp.concatenate([thermal_state[:, 1:], thermal_east], axis=1),
        jnp.concatenate([thermal_west, thermal_state[:, :-1]], axis=1),
        east,
        north,
    )

    water = water_indicator.astype(jnp.float32)
    cap = -(-3 * across * lat // 4 // LANES) * LANES
    wet = (water_indicator > 0).astype(jnp.int32).reshape(-1, LANES)
    within = jnp.cumsum(wet, axis=1) - wet
    count = jnp.sum(wet, axis=1)
    offset = jnp.cumsum(count) - count
    tiles = offset // LANES
    shifts = offset % LANES
    slot = within + shifts[:, None]
    lane = jnp.arange(LANES, dtype=jnp.int32)
    hit = (slot % LANES)[:, None, :] == lane[None, :, None]
    gather = jnp.sum(
        jnp.where(hit & (wet > 0)[:, None, :], lane[None, None, :], 0), axis=2, dtype=jnp.int32
    )
    spread_at = slot % LANES
    spread_later = slot // LANES

    speeds = linear_exchange_speeds.reshape(n, held, n, held)
    precon = newton_preconditioner.reshape(n, held, n, held)
    speeds = relative(relative(speeds, me, n, 0), me, n, 2).reshape(tracers, tracers)
    precon = relative(relative(precon, me, n, 0), me, n, 2).reshape(tracers, tracers)
    rates = relative(absorption_speed.reshape(n, held), me, n, 0).reshape(tracers)
    row = jnp.arange(tracers * ROWS, dtype=jnp.int32)
    copy = (row[:, None] // ROWS == jnp.arange(tracers)[None, :]).astype(jnp.float32)
    same = row[:, None] % ROWS == row[None, :] % ROWS

    def widened(x):
        x = jnp.dot(copy, x, precision=lax.Precision.HIGHEST)
        x = jnp.dot(x, copy.T, precision=lax.Precision.HIGHEST)
        return halves_of(jnp.where(same, x, 0.0))

    speeds = widened(speeds)
    precon = widened(precon)
    rates = jnp.dot(
        copy, jnp.broadcast_to(rates[:, None], (tracers, lat)), precision=lax.Precision.HIGHEST
    )

    fields = (east, north, kmix, water, speeds, precon, rates, gather)
    edges = {}
    for q in range(parts):
        level, turn = {0: (0, 1), parts - 1: (nl - 1, n - 1)}.get(q, (None, 0))
        edges[q] = list(chunk_edges(blocks[q], level, turn))
        edges[q][0] = around(edges[q][0], "col", -1)
        edges[q][1] = around(edges[q][1], "col", 1)
    if parts == 1:
        edges[0].append(jnp.concatenate([b[:, -1:] for b in blocks[0][-1:] + blocks[0][:-1]], 0))
    above_all = shifted(edges[0][2], "sec", -1)
    below_all = shifted(edges[parts - 1][-1], "sec", 1)

    absorbs = {}
    returned = {}
    total = jnp.zeros((across, lat), jnp.float32)
    for q in order:
        below = (blocks[q - 1], nl - 1) if q > 0 else (below_all, 0)
        above = (blocks[q + 1], 0) if q < parts - 1 else (above_all, 0)
        *packed, absorbs[q], total = react_chunk(
            q, nl, me_at, tiles, shifts, blocks[q], below, above, edges[q][:2], fields, total,
            cap, q == order[-1],
        )
        returned[q] = []
        for d, x in enumerate(packed):
            returned[q].append(around(x, "sec", -d) if d else x)

    absorb = jnp.concatenate([absorbs[q] for q in range(parts)], axis=0)
    sun = shortwave[None, :]

    small = (water, spread_at, spread_later)
    solute_revised = None
    for q in order:
        heat = (absorb, sun, thermal_carried) if q == order[-1] else ()
        solute_revised, *thermal_revised = unpack_chunk(
            q, parts, me_at, tiles, returned[q], solute_fields, small, solute_revised, cap, heat
        )
    return thermal_revised[0], jnp.stack([east, north]), spreading, solute_revised


def solution(mesh):
    placed = (
        P("sec", "col", None),
        P(None, "sec", "col", None),
        P("sec", "col", None),
        P("sec", None, "col", None),
        P(),
        P(),
        P(),
        P("col", None),
    )
    return jax.shard_map(
        on_device,
        mesh=mesh,
        in_specs=placed,
        out_specs=(
            P("sec", "col", None),
            P(None, "sec", "col", None),
            P("sec", "col", None),
            P("sec", None, "col", None),
        ),
        check_vma=False,
    )
```
